256 devices in a mesh: dp: 64 (over z, y, core), query: 4 (over x).
Axes of the slice: x: 4, y: 4, z: 8, core: 2. Of those that a mesh axis runs over, the one named last changes fastest.
Arguments:
- sensors: bfloat16 [24576, 4096], P('dp'), may hold values from -8 to 8
- query_index: int32 [2, 8192], P(None, 'query'), may hold values from 0 to 127
- targets: bfloat16 [24576, 8192], P('dp', 'query'), may hold values from -6 to 6
- w_one: bfloat16 [4096, 1024], P(None, 'query'), may hold values from -0.09375 to 0.09375
- b_one: float32 [1024], P('query'), may hold values from -3 to 3
- w_two: bfloat16 [1024, 512], P('query'), may hold values from -0.1875 to 0.1875
- b_two: float32 [512], replicated, may hold values from -3 to 3
- v_one: float32 [2, 512], replicated, may hold values from -4 to 4
- c_one: float32 [512], replicated, may hold values from -3 to 3
- v_two: bfloat16 [512, 512], replicated, may hold values from -0.25 to 0.25
- c_two: float32 [512], replicated, may hold values from -3 to 3
- v_three: bfloat16 [512, 512], replicated, may hold values from -0.25 to 0.25
- c_three: float32 [512], replicated, may hold values from -3 to 3
Outputs:
- loss: float32 [], replicated
- grad_w_one: float32 [4096, 1024], P('dp', 'query')
- grad_b_one: float32 [1024], P('query')
- grad_w_two: float32 [1024, 512], P('query', 'dp')
- grad_b_two: float32 [512], replicated
- grad_v_one: float32 [2, 512], replicated
- grad_c_one: float32 [512], replicated
- grad_v_two: float32 [512, 512], replicated
- grad_c_two: float32 [512], replicated
- grad_v_three: float32 [512, 512], replicated
- grad_c_three: float32 [512], replicated
The draws below stay inside these ranges and needn't reach their ends.
All inputs are finite; a program needn't handle non-finite values.
Results may differ from the reference program's by a relative error of at most 0.00075.
Values may be sent and summed in bfloat16 or wider, within the bound.
No kernel may reach another device: no remote copies, remote signals or barrier semaphores. Data moves between devices by JAX's collectives and lax.ppermute only.
A program may use at most 128 MiB of HBM per device.

```python
import math
import jax
import jax.numpy as jnp
from jax import lax

SENSORS = 4096
HIDDEN_SIZE = 1024
BASIS = 512
TRUNK = 512
GRID = 128
FUNC_DEV = 384
FUNCS = 24576
QUERIES = 8192
N_DP = 64


latent_count = 8


def joint_fields(key):
    key_latent = jax.random.fold_in(key, 7101)
    key_sdirs = jax.random.fold_in(key, 7102)
    key_qdirs = jax.random.fold_in(key, 7103)
    key_snoise = jax.random.fold_in(key, 7104)
    key_tnoise = jax.random.fold_in(key, 7105)
    key_pairs = jax.random.fold_in(key, 7107)
    latent = jax.random.normal(key_latent, (FUNCS, latent_count), jnp.float32)
    sensor_dirs = jax.random.normal(key_sdirs, (latent_count, SENSORS), jnp.float32)
    query_dirs = jax.random.normal(key_qdirs, (latent_count, QUERIES), jnp.float32)
    sensor_noise = jax.random.normal(key_snoise, (FUNCS, SENSORS), jnp.float32)
    target_noise = jax.random.normal(key_tnoise, (FUNCS, QUERIES), jnp.float32)
    noise_share = 0.5
    pairing = jax.random.permutation(key_pairs, N_DP)
    func_block = jnp.arange(FUNCS, dtype=jnp.int32) // FUNC_DEV
    sensor_block = jnp.arange(SENSORS, dtype=jnp.int32) // (SENSORS // N_DP)
    spiked = pairing[func_block][:, None] == sensor_block[None, :]
    boost = jnp.where(spiked, 3.0, 1.0).astype(jnp.float32)
    mixed = jnp.dot(latent, sensor_dirs) * (0.9 / math.sqrt(latent_count))
    sensors = jnp.clip(0.5 * boost * sensor_noise + mixed, -8.0, 8.0)
    solution = jnp.dot(latent, query_dirs) * (1.0 / math.sqrt(latent_count))
    targets = jnp.clip(solution + noise_share * target_noise, -6.0, 6.0)
    return (sensors, targets)


def draw_sensors(key, part):
    return joint_fields(key)[0].astype(jnp.bfloat16)


def draw_targets(key, part):
    return joint_fields(key)[1].astype(jnp.bfloat16)


def with_ends(drawn, rng, smallest, largest):
    spot = [jax.random.randint(jax.random.fold_in(rng, axis), (), 0, length) for axis, length in enumerate(drawn.shape)]
    widest = drawn.shape.index(max(drawn.shape))
    neighbour = spot[:widest] + [(spot[widest] + 1) % drawn.shape[widest]] + spot[widest + 1:]
    return drawn.at[tuple(spot)].set(smallest).at[tuple(neighbour)].set(largest)


def shard_levels(own_key, extent, split, smallest, high):
    def one(dim, parts):
        steps = jax.random.uniform(jax.random.fold_in(jax.random.fold_in(own_key, 6), dim), (parts,), jnp.float32, smallest / len(split), high / len(split))
        return jnp.repeat(jnp.exp(steps), extent[dim] // parts).reshape((-1,) + (1,) * (len(extent) - dim - 1))

    gain = one(*split[0])
    for cut in split[1:]:
        gain = gain * one(*cut)
    return gain


def normal_values(stream_key, extent, spread, reach, cuts=(), held_as=jnp.bfloat16):
    entries = spread * jax.random.normal(stream_key, extent, jnp.float32)
    if cuts:
        entries = entries * shard_levels(stream_key, extent, cuts, -0.22, 0.18)
    return jnp.clip(entries, -reach, reach).astype(held_as)


def setup_inputs(seed: int = 0) -> dict:
    streams_of = jax.random.split(jax.random.key(seed), 14)
    sensors = draw_sensors(jax.random.fold_in(streams_of[13], 71), 0)
    query_index = with_ends(jax.random.randint(streams_of[1], (2, QUERIES), 0, GRID), jax.random.fold_in(streams_of[1], 1), 0, GRID - 1).astype(jnp.int32)
    targets = draw_targets(jax.random.fold_in(streams_of[13], 71), 0)
    w_one = normal_values(streams_of[3], (SENSORS, HIDDEN_SIZE), SENSORS ** -0.5, 0.09375, ((1, 4),))
    b_one = normal_values(streams_of[4], (HIDDEN_SIZE,), 0.5, 3.0, ((0, 4),), jnp.float32)
    w_two = normal_values(streams_of[5], (HIDDEN_SIZE, BASIS), HIDDEN_SIZE ** -0.5, 0.1875, ((0, 4),))
    b_two = normal_values(streams_of[6], (BASIS,), 0.5, 3.0, (), jnp.float32)
    v_one = normal_values(streams_of[7], (2, TRUNK), 2 ** -0.5, 4.0, (), jnp.float32)
    c_one = normal_values(streams_of[8], (TRUNK,), 0.5, 3.0, (), jnp.float32)
    v_two = normal_values(streams_of[9], (TRUNK, TRUNK), TRUNK ** -0.5, 0.25)
    c_two = normal_values(streams_of[10], (TRUNK,), 0.5, 3.0, (), jnp.float32)
    v_three = normal_values(streams_of[11], (TRUNK, BASIS), TRUNK ** -0.5, 0.25)
    c_three = normal_values(streams_of[12], (BASIS,), 0.5, 3.0, (), jnp.float32)
    return {"sensors": sensors, "query_index": query_index, "targets": targets, "w_one": w_one, "b_one": b_one, "w_two": w_two, "b_two": b_two, "v_one": v_one, "c_one": c_one, "v_two": v_two, "c_two": c_two, "v_three": v_three, "c_three": c_three}


def contract_rows(left, right, precision=None):
    return lax.dot_general(left, right, (((0,), (0,)), ((), ())), precision=precision, preferred_element_type=jnp.float32)

def contract_cols(left, right, precision=None):
    return lax.dot_general(left, right, (((1,), (1,)), ((), ())), precision=precision, preferred_element_type=jnp.float32)

def trunk_forward(coords, v_one, c_one, v_two, c_two, v_three, c_three):
    first_act = jnp.tanh(coords[0][:, None] * v_one[0][None, :] + coords[1][:, None] * v_one[1][None, :] + c_one)
    first_b = first_act.astype(jnp.bfloat16)
    second_act = jnp.tanh(jnp.dot(first_b, v_two, preferred_element_type=jnp.float32) + c_two)
    second_b = second_act.astype(jnp.bfloat16)
    basis_full = jnp.dot(second_b, v_three, preferred_element_type=jnp.float32) + c_three
    return (first_act, first_b, second_act, second_b, basis_full.astype(jnp.bfloat16))

def trunk_backward(coords, first_act, first_b, second_act, second_b, grad_basis, v_two, v_three):
    grad_basis_b = grad_basis.astype(jnp.bfloat16)
    grad_v_three = contract_rows(second_b, grad_basis_b)
    grad_c_three = lax.optimization_barrier(jnp.sum(grad_basis, axis=0))
    grad_second = contract_cols(grad_basis_b, v_three) * (1.0 - second_act * second_act)
    grad_second_b = grad_second.astype(jnp.bfloat16)
    grad_v_two = contract_rows(first_b, grad_second_b)
    grad_c_two = lax.optimization_barrier(jnp.sum(grad_second, axis=0))
    grad_first = contract_cols(grad_second_b, v_two) * (1.0 - first_act * first_act)
    grad_v_one = jnp.dot(coords, grad_first, precision=lax.Precision.HIGHEST, preferred_element_type=jnp.float32)
    grad_c_one = lax.optimization_barrier(jnp.sum(grad_first, axis=0))
    return (grad_v_one, grad_c_one, grad_v_two, grad_c_two, grad_v_three, grad_c_three)

def reference(sensors, query_index, targets, w_one, b_one, w_two, b_two, v_one, c_one, v_two, c_two, v_three, c_three):
    coords = query_index.astype(jnp.float32) / (GRID - 1)
    first_act, first_b, second_act, second_b, basis_b = trunk_forward(coords, v_one, c_one, v_two, c_two, v_three, c_three)
    inv_scale = 1.0 / math.sqrt(BASIS)
    grad_scale = 64.0 / math.sqrt(FUNCS * QUERIES)
    sens_blocks = sensors.reshape(N_DP, FUNC_DEV, SENSORS)
    target_blocks = targets.reshape(N_DP, FUNC_DEV, QUERIES)

    def accumulate(running, block):
        loss_sum, grad_basis, grad_w_one, grad_b_one, grad_w_two, grad_b_two = running
        sens_block, target_block = block
        hidden = jnp.tanh(jnp.dot(sens_block, w_one, preferred_element_type=jnp.float32) + b_one)
        hidden_b = hidden.astype(jnp.bfloat16)
        coeffs = jnp.dot(hidden_b, w_two, preferred_element_type=jnp.float32) + b_two
        coeffs_b = coeffs.astype(jnp.bfloat16)
        prediction = contract_cols(coeffs_b, basis_b) * inv_scale
        misfit = prediction - target_block.astype(jnp.float32)
        loss_sum = loss_sum + jnp.sum(misfit * misfit)
        misfit_b = (misfit * grad_scale).astype(jnp.bfloat16)
        grad_coeffs = jnp.dot(misfit_b, basis_b, preferred_element_type=jnp.float32) * inv_scale
        grad_coeffs_b = grad_coeffs.astype(jnp.bfloat16)
        grad_basis = grad_basis + contract_rows(misfit_b, coeffs_b) * inv_scale
        grad_b_two = grad_b_two + lax.optimization_barrier(jnp.sum(grad_coeffs, axis=0))
        grad_w_two = grad_w_two + contract_rows(hidden_b, grad_coeffs_b)
        grad_pre = contract_cols(grad_coeffs_b, w_two) * (1.0 - hidden * hidden)
        grad_b_one = grad_b_one + lax.optimization_barrier(jnp.sum(grad_pre, axis=0))
        grad_w_one = grad_w_one + contract_rows(sens_block, grad_pre.astype(jnp.bfloat16))
        return ((loss_sum, grad_basis, grad_w_one, grad_b_one, grad_w_two, grad_b_two), None)
    initial = (jnp.zeros((), jnp.float32), jnp.zeros((QUERIES, BASIS), jnp.float32), jnp.zeros((SENSORS, HIDDEN_SIZE), jnp.float32), jnp.zeros((HIDDEN_SIZE,), jnp.float32), jnp.zeros((HIDDEN_SIZE, BASIS), jnp.float32), jnp.zeros((BASIS,), jnp.float32))
    final, _ = lax.scan(accumulate, initial, (sens_blocks, target_blocks))
    loss_sum, grad_basis, grad_w_one, grad_b_one, grad_w_two, grad_b_two = final
    grad_v_one, grad_c_one, grad_v_two, grad_c_two, grad_v_three, grad_c_three = trunk_backward(coords, first_act, first_b, second_act, second_b, grad_basis, v_two, v_three)
    return (loss_sum / (FUNCS * QUERIES), grad_w_one, grad_b_one, grad_w_two, grad_b_two, grad_v_one, grad_c_one, grad_v_two, grad_c_two, grad_v_three, grad_c_three)
```

```python
import math

import jax
import jax.numpy as jnp
from jax import lax
from jax.sharding import Mesh
from jax.sharding import PartitionSpec as P

GRID = 128
DP = ("z", "y", "c")
ALL = ("z", "y", "c", "query")


def shift(x, axis, k):
    n = lax.axis_size(axis)
    return lax.ppermute(x, axis, [(i, (i + k) % n) for i in range(n)])


def part(x, i):
    return lax.dynamic_index_in_dim(x, i, 0, False)


def scattered_sum(chunks, axis):
    n, i = lax.axis_size(axis), lax.axis_index(axis)
    arrived = [shift(part(chunks, (i + k) % n), axis, k) for k in range(1, n)]
    total = part(chunks, i)
    for a in arrived:
        total = total + a
    return total


def broadcast_sum(x, axis):
    pieces = gathered(x[None], axis)
    total = pieces[0]
    for j in range(1, lax.axis_size(axis)):
        total = total + pieces[j]
    return total


def gathered(x, axis):
    n, i, m = lax.axis_size(axis), lax.axis_index(axis), x.shape[0]
    pieces = [x] + [shift(x, axis, k) for k in range(1, n)]
    out = jnp.zeros((n * m, *x.shape[1:]), x.dtype)
    for k, piece in enumerate(pieces):
        out = lax.dynamic_update_slice_in_dim(out, piece, (i - k) % n * m, 0)
    return out


def contract_rows(left, right, precision=None):
    return lax.dot_general(
        left,
        right,
        (((0,), (0,)), ((), ())),
        precision=precision,
        preferred_element_type=jnp.float32,
    )


def contract_cols(left, right, precision=None):
    return lax.dot_general(
        left,
        right,
        (((1,), (1,)), ((), ())),
        precision=precision,
        preferred_element_type=jnp.float32,
    )


def trunk_forward(coords, v_one, c_one, v_two, c_two, v_three, c_three):
    first_act = jnp.tanh(
        coords[0][:, None] * v_one[0][None, :] + coords[1][:, None] * v_one[1][None, :] + c_one
    )
    first_b = first_act.astype(jnp.bfloat16)
    second_act = jnp.tanh(jnp.dot(first_b, v_two, preferred_element_type=jnp.float32) + c_two)
    second_b = second_act.astype(jnp.bfloat16)
    basis_full = jnp.dot(second_b, v_three, preferred_element_type=jnp.float32) + c_three
    return (first_act, first_b, second_act, second_b, basis_full.astype(jnp.bfloat16))


def trunk_backward(coords, first_act, first_b, second_act, second_b, grad_basis, v_two, v_three):
    grad_basis_b = grad_basis.astype(jnp.bfloat16)
    grad_v_three = contract_rows(second_b, grad_basis_b)
    grad_c_three = jnp.sum(grad_basis, axis=0)
    grad_second = contract_cols(grad_basis_b, v_three) * (1.0 - second_act * second_act)
    grad_second_b = grad_second.astype(jnp.bfloat16)
    grad_v_two = contract_rows(first_b, grad_second_b)
    grad_c_two = jnp.sum(grad_second, axis=0)
    grad_first = contract_cols(grad_second_b, v_two) * (1.0 - first_act * first_act)
    grad_v_one = jnp.dot(
        coords, grad_first, precision=lax.Precision.HIGHEST, preferred_element_type=jnp.float32
    )
    grad_c_one = jnp.sum(grad_first, axis=0)
    return (grad_v_one, grad_c_one, grad_v_two, grad_c_two, grad_v_three, grad_c_three)


def sum_of_all(big, small):
    rows, w = big.shape

    def cut(big, small, axis):
        n = lax.axis_size(axis)
        chunks = big.reshape(n, -1, w)
        chunks = jnp.concatenate([chunks, jnp.broadcast_to(small, (n, *small.shape))], axis=1)
        total = scattered_sum(chunks, axis)
        return total[:-8], total[-8:]

    for axis in ("c", "query", "z"):
        big, small = cut(big, small, axis)
    both = broadcast_sum(jnp.concatenate([big, small]), "y")
    big, small = both[:-8], both[-8:]
    for axis in ("z", "query", "c"):
        big = gathered(big, axis)
    return big, small


def local(
    sensors,
    query_index,
    targets,
    w_one,
    b_one,
    w_two,
    b_two,
    v_one,
    c_one,
    v_two,
    c_two,
    v_three,
    c_three,
):
    funcs, sensor_count = sensors.shape
    hidden_count, basis_count = w_two.shape
    trunk_count = v_two.shape[0]
    query_rows = query_index.shape[1]
    nz, ny, nc, nx = (lax.axis_size(a) for a in ALL)
    count_all = funcs * nz * ny * nc * query_rows * nx
    grad_scale = 64.0 / math.sqrt(count_all)
    inv_scale = 1.0 / math.sqrt(basis_count)
    iy, ix = lax.axis_index("y"), lax.axis_index("query")
    coords = query_index.astype(jnp.float32) / (GRID - 1)

    rows_own = sensor_count // (nz * ny * nc)
    columns = sensors.reshape(funcs, nz, ny, nc * rows_own)

    def columns_of(y):
        return lax.dynamic_index_in_dim(columns, y, 2, False).reshape(funcs, -1)

    sens_y = [columns_of(iy)] + [shift(columns_of((iy + k) % ny), "y", k) for k in range(1, ny)]

    hidden = jnp.tanh(jnp.dot(sensors, w_one, preferred_element_type=jnp.float32) + b_one)
    hidden_b = hidden.astype(jnp.bfloat16)
    partial_value = jnp.dot(hidden_b, w_two, preferred_element_type=jnp.float32)
    coeffs_own = scattered_sum(partial_value.reshape(nx, -1, basis_count), "query") + b_two
    coeffs_b = gathered(coeffs_own.astype(jnp.bfloat16), "query")
    first_act, first_b, second_act, second_b, basis = trunk_forward(
        coords, v_one, c_one, v_two, c_two, v_three, c_three
    )

    prediction = contract_cols(coeffs_b, basis) * inv_scale
    misfit = prediction - targets.astype(jnp.float32)
    loss_part = jnp.sum(misfit * misfit)
    misfit_b = (misfit * grad_scale).astype(jnp.bfloat16)
    grad_part = jnp.dot(misfit_b, basis, preferred_element_type=jnp.float32) * inv_scale
    grad_own = scattered_sum(grad_part.reshape(nx, -1, basis_count), "query")
    b_two_part = jnp.sum(grad_own, axis=0)
    grad_coeffs_b = gathered(grad_own.astype(jnp.bfloat16), "query")

    grad_basis_part = contract_rows(misfit_b, coeffs_b) * inv_scale
    g_v_one, g_c_one, g_v_two, g_c_two, g_v_three, g_c_three = trunk_backward(
        coords, first_act, first_b, second_act, second_b, grad_basis_part, v_two, v_three
    )
    small = jnp.concatenate(
        [
            g_v_one,
            jnp.stack([g_c_one, g_c_two, g_c_three, b_two_part]),
            jnp.broadcast_to(loss_part, (2, basis_count)),
        ]
    )
    big, small = sum_of_all(jnp.concatenate([g_v_three, g_v_two]), small)

    grad_pre = contract_cols(grad_coeffs_b, w_two) * (1.0 - hidden * hidden)
    b_one_part = jnp.sum(grad_pre, axis=0)
    grad_pre_b = grad_pre.astype(jnp.bfloat16)

    w_two_part = contract_rows(grad_coeffs_b, hidden_b).reshape(nz, ny, nc, -1, hidden_count)
    b_one_rows = jnp.pad(b_one_part[None], ((0, 7), (0, 0)))

    def with_bias(rows, n):
        rows = rows.reshape(n, -1, hidden_count)
        return jnp.concatenate([rows, jnp.broadcast_to(b_one_rows, (n, 8, hidden_count))], axis=1)

    both = scattered_sum(with_bias(w_two_part.transpose(2, 0, 1, 3, 4), nc), "c")
    w_two_part, b_one_rows = both[:-8].reshape(nz, ny, -1, hidden_count), both[-8:]
    both = scattered_sum(with_bias(w_two_part.transpose(1, 0, 2, 3), ny), "y")
    w_two_part, b_one_rows = both[:-8].reshape(nz, -1, hidden_count), both[-8:]

    pre_y = [grad_pre_b] + [shift(grad_pre_b, "y", k) for k in range(1, ny)]
    w_one_part = contract_rows(sens_y[0], pre_y[0])
    for k in range(1, ny):
        w_one_part = w_one_part + contract_rows(sens_y[k], pre_y[k])
    w_one_part = w_one_part.reshape(nz, nc, rows_own, hidden_count).transpose(1, 0, 2, 3)
    w_one_part = scattered_sum(w_one_part, "c")
    last = jnp.concatenate(
        [w_one_part, w_two_part, jnp.broadcast_to(b_one_rows, (nz, 8, hidden_count))], axis=1
    )
    last = scattered_sum(last, "z")
    grad_w_one = last[:rows_own]
    grad_w_two = last[rows_own:-8].T
    grad_b_one = last[-8]
    return (
        small[6, 0] / count_all,
        grad_w_one,
        grad_b_one,
        grad_w_two,
        small[5],
        small[:2],
        small[2],
        big[trunk_count:],
        small[3],
        big[:trunk_count],
        small[4],
    )


def solution(mesh):
    torus = Mesh(mesh.devices.reshape(8, 4, 2, mesh.shape["query"]), ALL)
    return jax.shard_map(
        local,
        mesh=torus,
        in_specs=(
            P(DP, None),
            P(None, "query"),
            P(DP, "query"),
            P(None, "query"),
            P("query"),
            P("query", None),
            P(),
            P(),
            P(),
            P(),
            P(),
            P(),
            P(),
        ),
        out_specs=(
            P(),
            P(DP, "query"),
            P("query"),
            P("query", DP),
            P(),
            P(),
            P(),
            P(),
            P(),
            P(),
            P(),
        ),
        check_vma=False,
    )
```

```python
import functools
import math

import jax
import jax.numpy as jnp
from jax import lax
from jax.experimental import pallas as pl
from jax.experimental.pallas import tpu as pltpu
from jax.sharding import Mesh
from jax.sharding import PartitionSpec as P


GRID = 128
DP = ("z", "y", "c")
ALL = ("z", "y", "c", "query")


def shift(x, axis, k):
    n = lax.axis_size(axis)
    return lax.ppermute(x, axis, [(i, (i + k) % n) for i in range(n)])


def part(x, i):
    return lax.dynamic_index_in_dim(x, i, 0, False)


def scattered_sum(chunks, axis):
    n, i = lax.axis_size(axis), lax.axis_index(axis)
    arrived = [shift(part(chunks, (i + k) % n), axis, k) for k in range(1, n)]
    total = part(chunks, i)
    for a in arrived:
        total = total + a
    return total


def exchanged(x, axis):
    return lax.all_to_all(x, axis, 0, 0, tiled=True)


def told_to_all(x, axis):
    return exchanged(jnp.broadcast_to(x[None], (lax.axis_size(axis), *x.shape)), axis)


def other_core(x):
    return lax.ppermute(x, "c", [(0, 1), (1, 0)])


def contract_rows(left, right, precision=None):
    return lax.dot_general(
        left,
        right,
        (((0,), (0,)), ((), ())),
        precision=precision,
        preferred_element_type=jnp.float32,
    )


def contract_cols(left, right, precision=None):
    return lax.dot_general(
        left,
        right,
        (((1,), (1,)), ((), ())),
        precision=precision,
        preferred_element_type=jnp.float32,
    )


def trunk_forward(coords, v_one, c_one, v_two, c_two, v_three, c_three):
    first_act = jnp.tanh(
        coords[0][:, None] * v_one[0][None, :] + coords[1][:, None] * v_one[1][None, :] + c_one
    )
    first_b = first_act.astype(jnp.bfloat16)
    second_act = jnp.tanh(jnp.dot(first_b, v_two, preferred_element_type=jnp.float32) + c_two)
    second_b = second_act.astype(jnp.bfloat16)
    basis_full = jnp.dot(second_b, v_three, preferred_element_type=jnp.float32) + c_three
    return basis_full.astype(jnp.bfloat16)


def back_kernel(core, coords, misfit, coeffs, rows_in, v_two, v_three, mine, give, acc3, acc2, accs, *, inv_scale):
    step = pl.program_id(0)

    @pl.when(step == 0)
    def _():
        acc3[...] = jnp.zeros_like(acc3)
        acc2[...] = jnp.zeros_like(acc2)
        accs[...] = jnp.zeros_like(accs)

    points = coords[...].T
    x, y = points[:, 0:1], points[:, 1:2]
    first = jnp.tanh(x * rows_in[0:1, :] + y * rows_in[1:2, :] + rows_in[2:3, :])
    first_b = first.astype(jnp.bfloat16)
    second = jnp.tanh(jnp.dot(first_b, v_two[...], preferred_element_type=jnp.float32) + rows_in[3:4, :])
    second_b = second.astype(jnp.bfloat16)
    grad = contract_rows(misfit[...], coeffs[...]) * inv_scale
    grad_b = grad.astype(jnp.bfloat16)
    acc3[...] += contract_rows(second_b, grad_b)
    accs[4:5, :] += jnp.sum(grad, axis=0, keepdims=True)
    grad = contract_cols(grad_b, v_three[...]) * (1.0 - second * second)
    grad_b = grad.astype(jnp.bfloat16)
    acc2[...] += contract_rows(first_b, grad_b)
    accs[3:4, :] += jnp.sum(grad, axis=0, keepdims=True)
    grad = contract_cols(grad_b, v_two[...]) * (1.0 - first * first)
    accs[2:3, :] += jnp.sum(grad, axis=0, keepdims=True)
    accs[0:1, :] += jnp.sum(x * grad, axis=0, keepdims=True)
    accs[1:2, :] += jnp.sum(y * grad, axis=0, keepdims=True)

    rows = acc3.shape[0]

    @pl.when(step == pl.num_programs(0) - 1)
    def _():
        mine[rows:, :] = accs[...]
        give[rows:, :] = accs[...]

        @pl.when(core[0] == 0)
        def _():
            mine[:rows, :] = acc3[...]
            give[:rows, :] = acc2[...]

        @pl.when(core[0] != 0)
        def _():
            mine[:rows, :] = acc2[...]
            give[:rows, :] = acc3[...]


def trunk_backward(core, coords, misfit_b, coeffs_b, v_one, c_one, v_two, c_two, v_three, inv_scale):
    queries = misfit_b.shape[1]
    funcs, basis = coeffs_b.shape
    trunk = v_two.shape[0]
    block = 512

    def whole(*shape):
        return pl.BlockSpec(shape, lambda i, core: (0,) * len(shape))

    rows_in = jnp.concatenate([v_one, c_one[None], c_two[None], jnp.zeros((4, trunk), jnp.float32)])
    out = jax.ShapeDtypeStruct((trunk + 8, basis), jnp.float32)
    return pl.pallas_call(
        functools.partial(back_kernel, inv_scale=inv_scale),
        grid_spec=pltpu.PrefetchScalarGridSpec(
            num_scalar_prefetch=1,
            grid=(queries // block,),
            in_specs=[
                pl.BlockSpec((8, block), lambda i, core: (0, i)),
                pl.BlockSpec((funcs, block), lambda i, core: (0, i)),
                whole(funcs, basis),
                whole(8, trunk),
                whole(trunk, trunk),
                whole(trunk, basis),
            ],
            out_specs=[whole(trunk + 8, basis), whole(trunk + 8, basis)],
            scratch_shapes=[
                pltpu.VMEM((trunk, basis), jnp.float32),
                pltpu.VMEM((trunk, trunk), jnp.float32),
                pltpu.VMEM((8, basis), jnp.float32),
            ],
        ),
        out_shape=[out, out],
        cost_estimate=pl.CostEstimate(flops=12 * queries * trunk * basis, bytes_accessed=8_000_000, transcendentals=2 * queries * trunk),
        compiler_params=pltpu.CompilerParams(vmem_limit_bytes=60 * 2**20),
        name="trunk_backward",
    )(core.reshape(1), coords, misfit_b, coeffs_b, rows_in, v_two, v_three)


def scaled(x, axes=None):
    top = jnp.max(jnp.abs(x), axis=axes, keepdims=True)
    e = jnp.clip(jnp.floor(jnp.log2(jnp.maximum(top, 1e-30))), -100.0, 127.0) - 14.0
    return x * jnp.exp2(-e), e


def power(e):
    return jnp.exp2(e.astype(jnp.float32))


def summed_in_pairs(x, axis):
    n, k = lax.axis_size(axis), 1
    while k < n:
        x = x + lax.ppermute(x, axis, [(i, i ^ k) for i in range(n)])
        k *= 2
    return x


def with_tail(out, j, big_e, piece, piece_e):
    rows, w = out.shape[1] - 8, out.shape[2]
    out[j, rows:, :] = jnp.zeros((8, w), jnp.float32)
    out[j, rows : rows + 1, : piece.shape[1]] = piece
    out[j, rows + 1 : rows + 2, :] = jnp.broadcast_to(big_e, (1, w))
    out[j, rows + 2 : rows + 3, :] = jnp.broadcast_to(piece_e, (1, w))


def plane_messages(mine, got, late, n):
    w = mine.shape[1]
    rows = mine.shape[0] - 8
    per = n // 8
    k = w // per

    def body(mine, got, late, out):
        big, big_e = scaled(mine[:rows, :] + got[:rows, :])
        small, small_e = scaled(mine[rows:, :] + got[rows:, :] + late[...], 1)
        out[:, : rows // n, :] = big.reshape(n, rows // n, w)
        for j in range(n):
            i, at = j // per, j % per * k
            with_tail(out, j, big_e, small[i : i + 1, at : at + k], small_e[i : i + 1])

    out = pl.pallas_call(
        body,
        out_shape=jax.ShapeDtypeStruct((n, rows // n + 8, w), jnp.float32),
        compiler_params=pltpu.CompilerParams(vmem_limit_bytes=12 * 2**20),
        name="plane_messages",
    )(mine, got, late)
    return out.astype(jnp.float16)


def total_message(both, side):
    rows, w = both.shape[0] - 8, both.shape[1]

    def body(both, out):
        big, big_e = scaled(both[:rows, :])
        small, small_e = scaled(both[rows : rows + 1, :side])
        out[0, :rows, :] = big
        with_tail(out, 0, big_e, small, small_e)

    out = pl.pallas_call(
        body,
        out_shape=jax.ShapeDtypeStruct((1, rows + 8, w), jnp.float32),
        compiler_params=pltpu.CompilerParams(vmem_limit_bytes=12 * 2**20),
        name="total_message",
    )(both)
    return out[0].astype(jnp.float16)


def z_messages(core, w_one_part, got, w_two_part, b_one_row):
    nz, _, rows, w = w_one_part.shape
    m = w_two_part.shape[1]

    def body(core, part, got, two, bias, out):
        one, one_e = scaled(part[:, 0] + got[...])
        two, two_e = scaled(two[...])
        bias, bias_e = scaled(bias[...])
        out[:, :rows, :] = one
        out[:, rows : rows + m, :] = two
        for j in range(nz):
            out[j, rows + m :, :] = jnp.zeros((8, w), jnp.float32)
            for i, row in enumerate((bias, bias_e, two_e, one_e)):
                out[j, rows + m + i : rows + m + i + 1, :] = jnp.broadcast_to(row.reshape(1, -1), (1, w))

    out = pl.pallas_call(
        body,
        grid_spec=pltpu.PrefetchScalarGridSpec(
            num_scalar_prefetch=1,
            grid=(1,),
            in_specs=[
                pl.BlockSpec((nz, 1, rows, w), lambda i, core: (0, core[0], 0, 0)),
                pl.BlockSpec((nz, rows, w), lambda i, core: (0, 0, 0)),
                pl.BlockSpec((nz, m, w), lambda i, core: (0, 0, 0)),
                pl.BlockSpec((1, w), lambda i, core: (0, 0)),
            ],
            out_specs=pl.BlockSpec((nz, rows + m + 8, w), lambda i, core: (0, 0, 0)),
        ),
        out_shape=jax.ShapeDtypeStruct((nz, rows + m + 8, w), jnp.float32),
        compiler_params=pltpu.CompilerParams(vmem_limit_bytes=12 * 2**20),
        name="z_messages",
    )(core.reshape(1), w_one_part, got, w_two_part, b_one_row)
    return out.astype(jnp.float16)


def read(got, rows, side):
    big = got[:, :rows].astype(jnp.float32) * power(got[:, rows + 1 : rows + 2, :1])
    small = got[:, rows, :side].astype(jnp.float32) * power(got[:, rows + 2, :1])
    return big, small


def finished(core, got, other, side):
    n, rows, w = got.shape[0], got.shape[1] - 8, got.shape[2]
    per = n // 8

    def body(core, got, other, one, two, v_one, c_one, c_two, c_three, b_two, loss):
        def put(zero, last):
            for x, out in ((zero, one), (last, two)):
                out[...] = (x[:, :rows, :] * jnp.exp2(x[:, rows + 1 : rows + 2, :])).reshape(n * rows, w)
            small = zero[:, rows : rows + 1, :side] * jnp.exp2(zero[:, rows + 2 : rows + 3, :side])
            more = last[:, rows : rows + 1, :side] * jnp.exp2(last[:, rows + 2 : rows + 3, :side])
            both = small + more
            for p in range(per):
                at = slice(p * side, (p + 1) * side)
                v_one[0:1, at] = small[p]
                v_one[1:2, at] = small[per + p]
                c_one[:, at] = small[2 * per + p]
                c_two[:, at] = small[3 * per + p]
                c_three[:, at] = small[4 * per + p]
                b_two[:, at] = both[5 * per + p]
                loss[:, at] = both[6 * per + p]

        @pl.when(core[0] == 0)
        def _():
            put(got, other)

        @pl.when(core[0] != 0)
        def _():
            put(other, got)

    def whole(*shape):
        return pl.BlockSpec(shape, lambda i, core: (0,) * len(shape))

    shapes = [(n * rows, w), (n * rows, w), (2, w)] + [(1, w)] * 5
    return pl.pallas_call(
        body,
        grid_spec=pltpu.PrefetchScalarGridSpec(
            num_scalar_prefetch=1,
            grid=(1,),
            in_specs=[whole(*got.shape), whole(*got.shape)],
            out_specs=[whole(*shape) for shape in shapes],
        ),
        out_shape=[jax.ShapeDtypeStruct(shape, jnp.float32) for shape in shapes],
        compiler_params=pltpu.CompilerParams(vmem_limit_bytes=24 * 2**20),
        name="finished",
    )(core.reshape(1), got, other)


def z_finished(got, rows):
    nz, all_rows, w = got.shape
    m = all_rows - rows - 8

    def body(got, one, two, bias):
        def part(lo, hi, e):
            total = got[0, lo:hi, :] * jnp.exp2(got[0, e : e + 1, :])
            for j in range(1, nz):
                total = total + got[j, lo:hi, :] * jnp.exp2(got[j, e : e + 1, :])
            return total

        k = rows + m
        one[...] = part(0, rows, k + 3)
        two[...] = part(rows, k, k + 2)
        bias[...] = part(k, k + 1, k + 1)

    return pl.pallas_call(
        body,
        out_shape=[jax.ShapeDtypeStruct(shape, jnp.float32) for shape in ((rows, w), (m, w), (1, w))],
        compiler_params=pltpu.CompilerParams(vmem_limit_bytes=12 * 2**20),
        name="z_finished",
    )(got)


def sum_of_all(mine, give, late):
    w = mine.shape[1]
    rows = mine.shape[0] - 8
    n = lax.axis_size("y") * lax.axis_size("query")
    per, side = rows // n, 8 * w // n
    plane = ("y", "query")
    got = other_core(give)

    got = exchanged(plane_messages(mine, got, late, n), plane)
    big, small = read(got, per, side)
    big, small = jnp.sum(big, axis=0), jnp.sum(small, axis=0)
    both = jnp.concatenate([big, jnp.pad(small[None], ((0, 7), (0, w - side)))])
    both = summed_in_pairs(both, "z")
    got = told_to_all(total_message(both, side), plane)
    other = other_core(got)
    return finished(
        lax.axis_index("c"), got.astype(jnp.float32), other.astype(jnp.float32), side
    )


def local(
    sensors,
    query_index,
    targets,
    w_one,
    b_one,
    w_two,
    b_two,
    v_one,
    c_one,
    v_two,
    c_two,
    v_three,
    c_three,
):
    funcs, sensor_count = sensors.shape
    hidden_count, basis_count = w_two.shape
    query_rows = query_index.shape[1]
    nz, ny, nc, nx = (lax.axis_size(a) for a in ALL)
    count_all = funcs * nz * ny * nc * query_rows * nx
    grad_scale = 64.0 / math.sqrt(count_all)
    inv_scale = 1.0 / math.sqrt(basis_count)
    coords = query_index.astype(jnp.float32) / (GRID - 1)

    w_two_all = [w_two] + [shift(w_two, "query", k) for k in range(1, nx)]
    hidden = jnp.tanh(jnp.dot(sensors, w_one, preferred_element_type=jnp.float32) + b_one)
    hidden_b = hidden.astype(jnp.bfloat16)
    hidden_all = [hidden_b] + [shift(hidden_b, "query", k) for k in range(1, nx)]
    basis = trunk_forward(
        coords, v_one, c_one, v_two, c_two, v_three, c_three
    )

    rows_own = sensor_count // (nz * ny * nc)
    iy = lax.axis_index("y")
    sensors_late, _ = lax.optimization_barrier((sensors, hidden_b))
    columns = sensors_late.reshape(funcs, nz, ny, nc * rows_own)

    def columns_of(y):
        return lax.dynamic_index_in_dim(columns, y, 2, False).reshape(funcs, -1)

    sens_y = [columns_of(iy)] + [
        shift(columns_of((iy + k) % ny), "y", k) for k in range(1, ny)
    ]

    coeffs = b_two
    for h, w in zip(hidden_all, w_two_all):
        coeffs = coeffs + jnp.dot(h, w, preferred_element_type=jnp.float32)
    coeffs_b = coeffs.astype(jnp.bfloat16)
    prediction = contract_cols(coeffs_b, basis) * inv_scale
    misfit = prediction - targets.astype(jnp.float32)
    loss_part = jnp.sum(misfit * misfit)
    misfit_b = (misfit * grad_scale).astype(jnp.bfloat16)
    grad_part = jnp.dot(misfit_b, basis, preferred_element_type=jnp.float32) * inv_scale
    grad_own = exchanged(grad_part.reshape(nx, -1, basis_count), "query")
    grad_own = jnp.sum(grad_own, axis=0)
    b_two_part = jnp.sum(grad_own, axis=0)
    grad_coeffs_b = told_to_all(grad_own.astype(jnp.bfloat16), "query").reshape(funcs, basis_count)

    ic = lax.axis_index("c")
    mine, give = trunk_backward(
        ic, jnp.pad(coords, ((0, 6), (0, 0))), misfit_b, coeffs_b, v_one, c_one, v_two, c_two, v_three, inv_scale
    )
    late = jnp.stack([b_two_part, jnp.broadcast_to(loss_part, (basis_count,))])
    totals = sum_of_all(mine, give, jnp.pad(late, ((5, 1), (0, 0))))
    g_v_three, g_v_two, g_v_one, g_c_one, g_c_two, g_c_three, g_b_two, loss = totals

    grad_pre = contract_cols(grad_coeffs_b, w_two) * (1.0 - hidden * hidden)
    b_one_part = jnp.sum(grad_pre, axis=0)
    grad_pre_b = grad_pre.astype(jnp.bfloat16)

    pre_y = [grad_pre_b] + [shift(grad_pre_b, "y", k) for k in range(1, ny)]

    w_two_part = contract_rows(grad_coeffs_b, hidden_b)
    w_two_part = w_two_part.reshape(nz, ny, nc, -1, hidden_count)
    b_one_rows = jnp.pad(b_one_part[None], ((0, 7), (0, 0)))

    def with_bias(rows, n):
        rows = rows.reshape(n, -1, hidden_count)
        bias = jnp.broadcast_to(b_one_rows, (n, 8, hidden_count))
        return jnp.concatenate([rows, bias], axis=1)

    both = scattered_sum(with_bias(w_two_part.transpose(2, 0, 1, 3, 4), nc), "c")
    w_two_part, b_one_rows = both[:-8].reshape(nz, ny, -1, hidden_count), both[-8:]
    both = scattered_sum(with_bias(w_two_part.transpose(1, 0, 2, 3), ny), "y")
    w_two_part, b_one_row = both[:-8].reshape(nz, -1, hidden_count), both[-8:-7]

    w_one_part = contract_rows(sens_y[0], pre_y[0])
    for k in range(1, ny):
        w_one_part = w_one_part + contract_rows(sens_y[k], pre_y[k])
    w_one_part = w_one_part.reshape(nz, nc, rows_own, hidden_count)
    got = other_core(lax.dynamic_index_in_dim(w_one_part, 1 - ic, 1, False))
    sent = z_messages(ic, w_one_part, got, w_two_part, b_one_row)
    got = exchanged(sent, "z")
    grad_w_one, grad_w_two, grad_b_one = z_finished(got.astype(jnp.float32), rows_own)
    return (
        loss[0, 0] / count_all,
        grad_w_one,
        grad_b_one[0],
        grad_w_two.T,
        g_b_two[0],
        g_v_one,
        g_c_one[0],
        g_v_two,
        g_c_two[0],
        g_v_three,
        g_c_three[0],
    )


def solution(mesh):
    torus = Mesh(mesh.devices.reshape(8, 4, 2, mesh.shape["query"]), ALL)
    return jax.shard_map(
        local,
        mesh=torus,
        in_specs=(
            P(DP, None),
            P(None, "query"),
            P(DP, "query"),
            P(None, "query"),
            P("query"),
            P("query", None),
            P(),
            P(),
            P(),
            P(),
            P(),
            P(),
            P(),
        ),
        out_specs=(
            P(),
            P(DP, "query"),
            P("query"),
            P("query", DP),
            P(),
            P(),
            P(),
            P(),
            P(),
            P(),
            P(),
        ),
        check_vma=False,
    )
```

```python
import functools
import math

import jax
import jax.numpy as jnp
from jax import lax
from jax.experimental import pallas as pl
from jax.experimental.pallas import tpu as pltpu
from jax.sharding import Mesh
from jax.sharding import PartitionSpec as P


GRID = 128
DP = ("z", "y", "c")
ALL = ("z", "y", "c", "query")


def shift(x, axis, k):
    n = lax.axis_size(axis)
    return lax.ppermute(x, axis, [(i, (i + k) % n) for i in range(n)])


def part(x, i):
    return lax.dynamic_index_in_dim(x, i, 0, False)


def scattered_sum(chunks, axis):
    n, i = lax.axis_size(axis), lax.axis_index(axis)
    arrived = [shift(part(chunks, (i + k) % n), axis, k) for k in range(1, n)]
    total = part(chunks, i)
    for a in arrived:
        total = total + a
    return total


def exchanged(x, axis):
    return lax.all_to_all(x, axis, 0, 0, tiled=True)


def other_core(x):
    return lax.ppermute(x, "c", [(0, 1), (1, 0)])


def contract_rows(left, right, precision=None):
    return lax.dot_general(
        left,
        right,
        (((0,), (0,)), ((), ())),
        precision=precision,
        preferred_element_type=jnp.float32,
    )


def contract_cols(left, right, precision=None):
    return lax.dot_general(
        left,
        right,
        (((1,), (1,)), ((), ())),
        precision=precision,
        preferred_element_type=jnp.float32,
    )


def points_of(index):
    coords = index.astype(jnp.float32) / (GRID - 1)
    columns = jnp.concatenate([coords, jnp.zeros((6, coords.shape[1]), jnp.float32)]).T
    return columns[:, 0:1], columns[:, 1:2]


def whole(*shape):
    return pl.BlockSpec(shape, lambda i, *_: (0,) * len(shape))


def trunk_forward(query_index, v_one, c_one, v_two, c_two, v_three, c_three):
    queries = query_index.shape[1]
    trunk, basis = v_three.shape
    block = 512

    def body(index, v_one, c_one, v_two, c_two, v_three, c_three, out, first_out, second_out):
        x, y = points_of(index[...])
        first = jnp.tanh(x * v_one[0:1, :] + y * v_one[1:2, :] + c_one[...])
        second = jnp.dot(first.astype(jnp.bfloat16), v_two[...], preferred_element_type=jnp.float32)
        second = jnp.tanh(second + c_two[...])
        first_out[...] = first
        second_out[...] = second
        full = jnp.dot(second.astype(jnp.bfloat16), v_three[...], preferred_element_type=jnp.float32) + c_three[...]
        out[...] = full.astype(jnp.bfloat16)

    return pl.pallas_call(
        body,
        grid=(queries // block,),
        in_specs=[
            pl.BlockSpec((2, block), lambda i: (0, i)),
            whole(2, trunk),
            whole(1, trunk),
            whole(trunk, trunk),
            whole(1, trunk),
            whole(trunk, basis),
            whole(1, basis),
        ],
        out_specs=[
            pl.BlockSpec((block, basis), lambda i: (i, 0)),
            pl.BlockSpec((block, trunk), lambda i: (i, 0)),
            pl.BlockSpec((block, trunk), lambda i: (i, 0)),
        ],
        out_shape=[
            jax.ShapeDtypeStruct((queries, basis), jnp.bfloat16),
            jax.ShapeDtypeStruct((queries, trunk), jnp.float32),
            jax.ShapeDtypeStruct((queries, trunk), jnp.float32),
        ],
        cost_estimate=pl.CostEstimate(flops=4 * queries * trunk * basis, bytes_accessed=4_000_000, transcendentals=2 * queries * trunk),
        compiler_params=pltpu.CompilerParams(vmem_limit_bytes=60 * 2**20),
        name="trunk_forward",
    )(query_index, v_one, c_one[None], v_two, c_two[None], v_three, c_three[None])


def misfit_of(hidden_all, w_two_all, b_two, basis, targets, inv_scale, grad_scale):
    n = len(hidden_all)
    funcs, queries = targets.shape
    width = basis.shape[1]
    block = 512

    def body(*refs):
        hidden, w_two = refs[:n], refs[n : 2 * n]
        b_two, basis, targets, coeffs, misfit_b, squares, grad = refs[2 * n :]

        @pl.when(pl.program_id(0) == 0)
        def _():
            total = b_two[...]
            for h, w in zip(hidden, w_two):
                total = total + jnp.dot(h[...], w[...], preferred_element_type=jnp.float32)
            coeffs[...] = total.astype(jnp.bfloat16)
            squares[...] = jnp.zeros_like(squares)
            grad[...] = jnp.zeros_like(grad)

        misfit = contract_cols(coeffs[...], basis[...]) * inv_scale - targets[...].astype(jnp.float32)
        squares[...] += jnp.sum(misfit * misfit, axis=0, keepdims=True)
        scaled_b = (misfit * grad_scale).astype(jnp.bfloat16)
        misfit_b[...] = scaled_b
        grad[...] += jnp.dot(scaled_b, basis[...], preferred_element_type=jnp.float32) * inv_scale

    return pl.pallas_call(
        body,
        grid=(queries // block,),
        in_specs=[whole(*h.shape) for h in hidden_all]
        + [whole(*w.shape) for w in w_two_all]
        + [
            whole(1, width),
            pl.BlockSpec((block, width), lambda i: (i, 0)),
            pl.BlockSpec((funcs, block), lambda i: (0, i)),
        ],
        out_specs=[
            whole(funcs, width),
            pl.BlockSpec((funcs, block), lambda i: (0, i)),
            whole(1, block),
            whole(funcs, width),
        ],
        out_shape=[
            jax.ShapeDtypeStruct((funcs, width), jnp.bfloat16),
            jax.ShapeDtypeStruct((funcs, queries), jnp.bfloat16),
            jax.ShapeDtypeStruct((1, block), jnp.float32),
            jax.ShapeDtypeStruct((funcs, width), jnp.float32),
        ],
        cost_estimate=pl.CostEstimate(flops=5 * funcs * queries * width, bytes_accessed=8_000_000, transcendentals=0),
        compiler_params=pltpu.CompilerParams(vmem_limit_bytes=60 * 2**20),
        name="misfit_of",
    )(*hidden_all, *w_two_all, b_two[None], basis, targets)


def pre_of(ix, pieces, hidden, w_two):
    n = len(pieces)
    rows, basis = pieces[0].shape
    funcs, width = hidden.shape

    def body(ix, *refs):
        hidden, w_two, pre_b, bias, product, grad = refs[n:]
        for k in range(n):
            at = lax.rem(ix[0] + n - k, n) * rows
            grad[pl.ds(pl.multiple_of(at, rows), rows), :] = refs[k][...]
        act = hidden[...]
        pre = contract_cols(grad[...], w_two[...]) * (1.0 - act * act)
        pre_b[...] = pre.astype(jnp.bfloat16)
        bias[...] = jnp.sum(pre, axis=0, keepdims=True)
        product[...] = contract_rows(grad[...], act.astype(jnp.bfloat16))

    return pl.pallas_call(
        body,
        grid_spec=pltpu.PrefetchScalarGridSpec(
            num_scalar_prefetch=1,
            grid=(1,),
            in_specs=[whole(rows, basis)] * n + [whole(funcs, width), whole(width, basis)],
            out_specs=[whole(funcs, width), whole(1, width), whole(basis, width)],
            scratch_shapes=[pltpu.VMEM((funcs, basis), jnp.bfloat16)],
        ),
        out_shape=[
            jax.ShapeDtypeStruct((funcs, width), jnp.bfloat16),
            jax.ShapeDtypeStruct((1, width), jnp.float32),
            jax.ShapeDtypeStruct((basis, width), jnp.float32),
        ],
        cost_estimate=pl.CostEstimate(flops=4 * funcs * basis * width, bytes_accessed=2_000_000, transcendentals=0),
        compiler_params=pltpu.CompilerParams(vmem_limit_bytes=12 * 2**20),
        name="pre_of",
    )(ix.reshape(1), *pieces, hidden, w_two)


def columns_by_y(sensors, iy, nz, ny, width):
    funcs = sensors.shape[0]

    def body(y, *refs):
        for src, dst in zip(refs[:ny], refs[ny:]):
            dst[...] = src[...].T

    def source(k):
        return pl.BlockSpec((funcs, width), lambda z, y: (0, z * ny + lax.rem(y[0] + k, ny)))

    return pl.pallas_call(
        body,
        grid_spec=pltpu.PrefetchScalarGridSpec(
            num_scalar_prefetch=1,
            grid=(nz,),
            in_specs=[source(k) for k in range(ny)],
            out_specs=[pl.BlockSpec((width, funcs), lambda z, y: (z, 0))] * ny,
        ),
        out_shape=[jax.ShapeDtypeStruct((nz * width, funcs), sensors.dtype)] * ny,
        cost_estimate=pl.CostEstimate(flops=8_000_000, bytes_accessed=4 * sensors.size, transcendentals=0),
        compiler_params=pltpu.CompilerParams(vmem_limit_bytes=60 * 2**20),
        name="columns_by_y",
    )(iy.reshape(1), *[sensors] * ny)


def back_kernel(core, index, misfit, coeffs, first_act, second_act, v_two, v_three, mine, give, acc3, acc2, accs, *, inv_scale):
    step = pl.program_id(0)

    @pl.when(step == 0)
    def _():
        acc3[...] = jnp.zeros_like(acc3)
        acc2[...] = jnp.zeros_like(acc2)
        accs[...] = jnp.zeros_like(accs)

    x, y = points_of(index[...])
    first, second = first_act[...], second_act[...]
    first_b, second_b = first.astype(jnp.bfloat16), second.astype(jnp.bfloat16)
    grad = contract_rows(misfit[...], coeffs[...]) * inv_scale
    grad_b = grad.astype(jnp.bfloat16)
    acc3[...] += contract_rows(second_b, grad_b)
    accs[4:5, :] += jnp.sum(grad, axis=0, keepdims=True)
    grad = contract_cols(grad_b, v_three[...]) * (1.0 - second * second)
    grad_b = grad.astype(jnp.bfloat16)
    acc2[...] += contract_rows(first_b, grad_b)
    accs[3:4, :] += jnp.sum(grad, axis=0, keepdims=True)
    grad = contract_cols(grad_b, v_two[...]) * (1.0 - first * first)
    accs[2:3, :] += jnp.sum(grad, axis=0, keepdims=True)
    accs[0:1, :] += jnp.sum(x * grad, axis=0, keepdims=True)
    accs[1:2, :] += jnp.sum(y * grad, axis=0, keepdims=True)

    rows = acc3.shape[0]

    @pl.when(step == pl.num_programs(0) - 1)
    def _():
        mine[rows:, :] = accs[...]
        give[rows:, :] = accs[...]

        @pl.when(core[0] == 0)
        def _():
            mine[:rows, :] = acc3[...]
            give[:rows, :] = acc2[...]

        @pl.when(core[0] != 0)
        def _():
            mine[:rows, :] = acc2[...]
            give[:rows, :] = acc3[...]


def trunk_backward(core, query_index, misfit_b, coeffs_b, first_act, second_act, v_two, v_three, inv_scale):
    queries = misfit_b.shape[1]
    funcs, basis = coeffs_b.shape
    trunk = v_two.shape[0]
    block = 512

    out = jax.ShapeDtypeStruct((trunk + 8, basis), jnp.float32)
    return pl.pallas_call(
        functools.partial(back_kernel, inv_scale=inv_scale),
        grid_spec=pltpu.PrefetchScalarGridSpec(
            num_scalar_prefetch=1,
            grid=(queries // block,),
            in_specs=[
                pl.BlockSpec((2, block), lambda i, core: (0, i)),
                pl.BlockSpec((funcs, block), lambda i, core: (0, i)),
                whole(funcs, basis),
                pl.BlockSpec((block, trunk), lambda i, core: (i, 0)),
                pl.BlockSpec((block, trunk), lambda i, core: (i, 0)),
                whole(trunk, trunk),
                whole(trunk, basis),
            ],
            out_specs=[whole(trunk + 8, basis), whole(trunk + 8, basis)],
            scratch_shapes=[
                pltpu.VMEM((trunk, basis), jnp.float32),
                pltpu.VMEM((trunk, trunk), jnp.float32),
                pltpu.VMEM((8, basis), jnp.float32),
            ],
        ),
        out_shape=[out, out],
        cost_estimate=pl.CostEstimate(flops=12 * queries * trunk * basis, bytes_accessed=8_000_000, transcendentals=2 * queries * trunk),
        compiler_params=pltpu.CompilerParams(vmem_limit_bytes=60 * 2**20),
        name="trunk_backward",
    )(core.reshape(1), query_index, misfit_b, coeffs_b, first_act, second_act, v_two, v_three)


def scaled(x, axes=None):
    top = jnp.max(jnp.abs(x), axis=axes, keepdims=True)
    e = jnp.clip(jnp.floor(jnp.log2(jnp.maximum(top, 1e-30))), -100.0, 127.0) - 14.0
    return x * jnp.exp2(-e), e


def summed_in_pairs(x, axis):
    n, k = lax.axis_size(axis), 1
    while k < n:
        x = x + lax.ppermute(x, axis, [(i, i ^ k) for i in range(n)])
        k *= 2
    return x


def with_tail(out, j, big_e, piece, piece_e):
    rows, w = out.shape[1] - 8, out.shape[2]
    out[j, rows:, :] = jnp.zeros((8, w), jnp.float32)
    out[j, rows : rows + 1, : piece.shape[1]] = piece
    out[j, rows + 1 : rows + 2, :] = jnp.broadcast_to(big_e, (1, w))
    out[j, rows + 2 : rows + 3, :] = jnp.broadcast_to(piece_e, (1, w))


def plane_messages(mine, got, b_two, squares, n):
    w = mine.shape[1]
    rows = mine.shape[0] - 8
    per = n // 8
    k = w // per

    def body(mine, got, b_two, squares, out):
        big, big_e = scaled(mine[:rows, :] + got[:rows, :])
        row = lax.broadcasted_iota(jnp.int32, (8, w), 0)
        small = mine[rows:, :] + got[rows:, :]
        small = jnp.where(row == 5, b_two[...], jnp.where(row == 6, squares[...], small))
        small, small_e = scaled(small, 1)
        out[:, : rows // n, :] = big.reshape(n, rows // n, w)
        for j in range(n):
            i, at = j // per, j % per * k
            with_tail(out, j, big_e, small[i : i + 1, at : at + k], small_e[i : i + 1])

    out = pl.pallas_call(
        body,
        out_shape=jax.ShapeDtypeStruct((n, rows // n + 8, w), jnp.float32),
        compiler_params=pltpu.CompilerParams(vmem_limit_bytes=12 * 2**20),
        name="plane_messages",
    )(mine, got, b_two, squares)
    return out.astype(jnp.float16)


def plane_total(got):
    n, rows, w = got.shape[0], got.shape[1] - 8, got.shape[2]

    def body(got, out):
        def total(lo, hi, e):
            x = got[0, lo:hi, :] * jnp.exp2(got[0, e : e + 1, :])
            for j in range(1, n):
                x = x + got[j, lo:hi, :] * jnp.exp2(got[j, e : e + 1, :])
            return x

        out[:rows, :] = total(0, rows, rows + 1)
        out[rows:, :] = jnp.zeros((8, w), jnp.float32)
        out[rows : rows + 1, :] = total(rows, rows + 1, rows + 2)

    return pl.pallas_call(
        body,
        out_shape=jax.ShapeDtypeStruct((rows + 8, w), jnp.float32),
        compiler_params=pltpu.CompilerParams(vmem_limit_bytes=12 * 2**20),
        name="plane_total",
    )(got)


def total_message(both, side):
    rows, w = both.shape[0] - 8, both.shape[1]

    def body(both, out):
        big, big_e = scaled(both[:rows, :])
        small, small_e = scaled(both[rows : rows + 1, :side])
        out[0, :rows, :] = big
        with_tail(out, 0, big_e, small, small_e)

    out = pl.pallas_call(
        body,
        out_shape=jax.ShapeDtypeStruct((1, rows + 8, w), jnp.float32),
        compiler_params=pltpu.CompilerParams(vmem_limit_bytes=12 * 2**20),
        name="total_message",
    )(both)
    return out[0].astype(jnp.float16)


def z_messages(core, w_one_part, got, w_two_part, b_one_row):
    nz, _, rows, w = w_one_part.shape
    m = w_two_part.shape[1]

    def body(core, part, got, two, bias, out):
        one, one_e = scaled(part[:, 0] + got[...])
        two, two_e = scaled(two[...])
        bias, bias_e = scaled(bias[...])
        out[:, :rows, :] = one
        out[:, rows : rows + m, :] = two
        for j in range(nz):
            out[j, rows + m :, :] = jnp.zeros((8, w), jnp.float32)
            for i, row in enumerate((bias, bias_e, two_e, one_e)):
                out[j, rows + m + i : rows + m + i + 1, :] = jnp.broadcast_to(row.reshape(1, -1), (1, w))

    out = pl.pallas_call(
        body,
        grid_spec=pltpu.PrefetchScalarGridSpec(
            num_scalar_prefetch=1,
            grid=(1,),
            in_specs=[
                pl.BlockSpec((nz, 1, rows, w), lambda i, core: (0, core[0], 0, 0)),
                pl.BlockSpec((nz, rows, w), lambda i, core: (0, 0, 0)),
                pl.BlockSpec((nz, m, w), lambda i, core: (0, 0, 0)),
                pl.BlockSpec((1, w), lambda i, core: (0, 0)),
            ],
            out_specs=pl.BlockSpec((nz, rows + m + 8, w), lambda i, core: (0, 0, 0)),
        ),
        out_shape=jax.ShapeDtypeStruct((nz, rows + m + 8, w), jnp.float32),
        compiler_params=pltpu.CompilerParams(vmem_limit_bytes=12 * 2**20),
        name="z_messages",
    )(core.reshape(1), w_one_part, got, w_two_part, b_one_row)
    return out.astype(jnp.float16)


def finished(place, got, other, side, ny, nx):
    n, rows, w = got.shape[0], got.shape[1] - 8, got.shape[2]
    per = n // 8

    def body(place, got, other, one, two, v_one, c_one, c_two, c_three, b_two, loss, small, more):
        def put(zero, last):
            for q in range(n):
                at = lax.rem(place[1] + ny - q // nx, ny) * nx + lax.rem(place[2] + nx - q % nx, nx)
                into = pl.ds(pl.multiple_of(at * rows, rows), rows)
                for x, out, part in ((zero, one, small), (last, two, more)):
                    out[into, :] = x[q, :rows, :] * jnp.exp2(x[q, rows + 1 : rows + 2, :])
                    part[pl.ds(at, 1), :] = x[q, rows : rows + 1, :side] * jnp.exp2(
                        x[q, rows + 2 : rows + 3, :side]
                    )

        @pl.when(place[0] == 0)
        def _():
            put(got, other)

        @pl.when(place[0] != 0)
        def _():
            put(other, got)

        total = jnp.zeros((1, 1), jnp.float32)
        for p in range(per):
            at = slice(p * side, (p + 1) * side)
            for i, (out, j) in enumerate(((v_one, 0), (v_one, 1), (c_one, 0), (c_two, 0), (c_three, 0))):
                out[j : j + 1, at] = small[i * per + p : i * per + p + 1, :]
            k = 5 * per + p
            b_two[:, at] = small[k : k + 1, :] + more[k : k + 1, :]
            k = 6 * per + p
            total = total + jnp.sum(small[k : k + 1, :] + more[k : k + 1, :], axis=1, keepdims=True)
        loss[...] = total

    shapes = [(n * rows, w), (n * rows, w), (2, w)] + [(1, w)] * 4 + [(1, 1)]
    return pl.pallas_call(
        body,
        grid_spec=pltpu.PrefetchScalarGridSpec(
            num_scalar_prefetch=1,
            grid=(1,),
            in_specs=[whole(*got.shape), whole(*got.shape)],
            out_specs=[whole(*shape) for shape in shapes],
            scratch_shapes=[pltpu.VMEM((n, side), jnp.float32)] * 2,
        ),
        out_shape=[jax.ShapeDtypeStruct(shape, jnp.float32) for shape in shapes],
        compiler_params=pltpu.CompilerParams(vmem_limit_bytes=24 * 2**20),
        name="finished",
    )(place, got, other)


def z_finished(got, rows):
    nz, all_rows, w = got.shape
    m = all_rows - rows - 8

    def body(got, one, two, bias):
        def part(lo, hi, e):
            total = got[0, lo:hi, :] * jnp.exp2(got[0, e : e + 1, :])
            for j in range(1, nz):
                total = total + got[j, lo:hi, :] * jnp.exp2(got[j, e : e + 1, :])
            return total

        k = rows + m
        one[...] = part(0, rows, k + 3)
        two[...] = part(rows, k, k + 2)
        bias[...] = part(k, k + 1, k + 1)

    return pl.pallas_call(
        body,
        out_shape=[jax.ShapeDtypeStruct(shape, jnp.float32) for shape in ((rows, w), (m, w), (1, w))],
        compiler_params=pltpu.CompilerParams(vmem_limit_bytes=12 * 2**20),
        name="z_finished",
    )(got)


def sum_of_all(mine, give, b_two, squares):
    w = mine.shape[1]
    ny, nx = lax.axis_size("y"), lax.axis_size("query")
    n = ny * nx
    side = 8 * w // n
    got = other_core(give)

    got = exchanged(plane_messages(mine, got, b_two, squares, n), ("y", "query"))
    both = plane_total(got.astype(jnp.float32))
    both = summed_in_pairs(both, "z")
    got = total_message(both, side)
    got = jnp.stack([got] + [shift(got, "query", k) for k in range(1, nx)])
    got = jnp.concatenate([got] + [shift(got, "y", k) for k in range(1, ny)])
    other = other_core(got)
    place = jnp.stack([lax.axis_index(a) for a in ("c", "y", "query")])
    return finished(
        place, got.astype(jnp.float32), other.astype(jnp.float32), side, ny, nx
    )


def local(
    sensors,
    query_index,
    targets,
    w_one,
    b_one,
    w_two,
    b_two,
    v_one,
    c_one,
    v_two,
    c_two,
    v_three,
    c_three,
):
    funcs, sensor_count = sensors.shape
    hidden_count, basis_count = w_two.shape
    query_rows = query_index.shape[1]
    nz, ny, nc, nx = (lax.axis_size(a) for a in ALL)
    count_all = funcs * nz * ny * nc * query_rows * nx
    grad_scale = 64.0 / math.sqrt(count_all)
    inv_scale = 1.0 / math.sqrt(basis_count)

    w_two_all = [w_two] + [shift(w_two, "query", k) for k in range(1, nx)]
    hidden = jnp.tanh(jnp.dot(sensors, w_one, preferred_element_type=jnp.float32) + b_one)
    hidden_b = hidden.astype(jnp.bfloat16)
    hidden_all = [hidden_b] + [shift(hidden_b, "query", k) for k in range(1, nx)]
    basis, first_act, second_act = trunk_forward(
        query_index, v_one, c_one, v_two, c_two, v_three, c_three
    )

    rows_own = sensor_count // (nz * ny * nc)
    iy, ic = lax.axis_index("y"), lax.axis_index("c")
    sensors_late, _ = lax.optimization_barrier((sensors, hidden_b))
    sens_y = columns_by_y(sensors_late, iy, nz, ny, nc * rows_own)
    sens_y = [sens_y[0]] + [shift(sens_y[k], "y", k) for k in range(1, ny)]

    coeffs_b, misfit_b, squares, grad_part = misfit_of(
        hidden_all, w_two_all, b_two, basis, targets, inv_scale, grad_scale
    )
    grad_own = exchanged(grad_part.reshape(nx, -1, basis_count), "query")
    grad_own = jnp.sum(grad_own, axis=0)
    b_two_part = jnp.sum(grad_own, axis=0, keepdims=True)
    grad_own_b = grad_own.astype(jnp.bfloat16)
    grad_pieces = [grad_own_b] + [shift(grad_own_b, "query", k) for k in range(1, nx)]

    mine, give = trunk_backward(ic, query_index, misfit_b, coeffs_b, first_act, second_act, v_two, v_three, inv_scale)
    totals = sum_of_all(mine, give, b_two_part, squares)
    g_v_three, g_v_two, g_v_one, g_c_one, g_c_two, g_c_three, g_b_two, loss = totals

    grad_pre_b, b_one_part, w_two_part = pre_of(
        lax.axis_index("query"), grad_pieces, hidden, w_two
    )

    pre_y = [grad_pre_b] + [shift(grad_pre_b, "y", k) for k in range(1, ny)]

    w_two_part = w_two_part.reshape(nz, ny, nc, -1, hidden_count)
    b_one_rows = jnp.pad(b_one_part, ((0, 7), (0, 0)))

    def with_bias(rows, n):
        rows = rows.reshape(n, -1, hidden_count)
        bias = jnp.broadcast_to(b_one_rows, (n, 8, hidden_count))
        return jnp.concatenate([rows, bias], axis=1)

    both = scattered_sum(with_bias(w_two_part.transpose(2, 0, 1, 3, 4), nc), "c")
    w_two_part, b_one_rows = both[:-8].reshape(nz, ny, -1, hidden_count), both[-8:]
    both = scattered_sum(with_bias(w_two_part.transpose(1, 0, 2, 3), ny), "y")
    w_two_part, b_one_row = both[:-8].reshape(nz, -1, hidden_count), both[-8:-7]

    w_one_part = jnp.dot(sens_y[0], pre_y[0], preferred_element_type=jnp.float32)
    for k in range(1, ny):
        w_one_part = w_one_part + jnp.dot(
            sens_y[k], pre_y[k], preferred_element_type=jnp.float32
        )
    w_one_part = w_one_part.reshape(nz, nc, rows_own, hidden_count)
    got = other_core(lax.dynamic_index_in_dim(w_one_part, 1 - ic, 1, False))
    sent = z_messages(ic, w_one_part, got, w_two_part, b_one_row)
    got = exchanged(sent, "z")
    grad_w_one, grad_w_two, grad_b_one = z_finished(got.astype(jnp.float32), rows_own)
    return (
        loss[0, 0] / count_all,
        grad_w_one,
        grad_b_one[0],
        grad_w_two.T,
        g_b_two[0],
        g_v_one,
        g_c_one[0],
        g_v_two,
        g_c_two[0],
        g_v_three,
        g_c_three[0],
    )


def solution(mesh):
    torus = Mesh(mesh.devices.reshape(8, 4, 2, mesh.shape["query"]), ALL)
    return jax.shard_map(
        local,
        mesh=torus,
        in_specs=(
            P(DP, None),
            P(None, "query"),
            P(DP, "query"),
            P(None, "query"),
            P("query"),
            P("query", None),
            P(),
            P(),
            P(),
            P(),
            P(),
            P(),
            P(),
        ),
        out_specs=(
            P(),
            P(DP, "query"),
            P("query"),
            P("query", DP),
            P(),
            P(),
            P(),
            P(),
            P(),
            P(),
            P(),
        ),
        check_vma=False,
    )
```

```python
import functools
import math

import jax
import jax.numpy as jnp
from jax import lax
from jax.experimental import pallas as pl
from jax.experimental.pallas import tpu as pltpu
from jax.sharding import Mesh
from jax.sharding import PartitionSpec as P


GRID = 128
BLOCK = 1024
CUT = 1024
DP = ("z", "y", "c")
ALL = ("z", "y", "c", "query")


def shift(x, axis, k):
    n = lax.axis_size(axis)
    return lax.ppermute(x, axis, [(i, (i + k) % n) for i in range(n)])


def part(x, i):
    return lax.dynamic_index_in_dim(x, i, 0, False)


def scattered_sum(chunks, axis):
    n, i = lax.axis_size(axis), lax.axis_index(axis)
    arrived = [shift(part(chunks, (i + k) % n), axis, k) for k in range(1, n)]
    total = part(chunks, i)
    for a in arrived:
        total = total + a
    return total


def exchanged(x, axis):
    return lax.all_to_all(x, axis, 0, 0, tiled=True)


def other_core(x):
    return lax.ppermute(x, "c", [(0, 1), (1, 0)])


def contract_rows(left, right, precision=None):
    return lax.dot_general(
        left,
        right,
        (((0,), (0,)), ((), ())),
        precision=precision,
        preferred_element_type=jnp.float32,
    )


def contract_cols(left, right, precision=None):
    return lax.dot_general(
        left,
        right,
        (((1,), (1,)), ((), ())),
        precision=precision,
        preferred_element_type=jnp.float32,
    )


def points_of(index):
    coords = index.astype(jnp.float32) / (GRID - 1)
    columns = jnp.concatenate([coords, jnp.zeros((6, coords.shape[1]), jnp.float32)]).T
    return columns[:, 0:1], columns[:, 1:2]


def whole(*shape):
    return pl.BlockSpec(shape, lambda i, *_: (0,) * len(shape))


def trunk_forward(query_index, v_one, c_one, v_two, c_two, v_three, c_three):
    queries = query_index.shape[1]
    trunk, basis = v_three.shape
    block = BLOCK

    def body(index, v_one, c_one, v_two, c_two, v_three, c_three, out, first_out, second_out):
        x, y = points_of(index[...])
        cuts = [slice(at, at + CUT) for at in range(0, block, CUT)]
        firsts = [
            jnp.tanh(x[c] * v_one[0:1, :] + y[c] * v_one[1:2, :] + c_one[...]) for c in cuts
        ]
        seconds = [
            jnp.dot(first.astype(jnp.bfloat16), v_two[...], preferred_element_type=jnp.float32)
            for first in firsts
        ]
        seconds = [jnp.tanh(second + c_two[...]) for second in seconds]
        for c, first, second in zip(cuts, firsts, seconds):
            first_out[c, :] = first
            second_out[c, :] = second
            full = jnp.dot(
                second.astype(jnp.bfloat16), v_three[...], preferred_element_type=jnp.float32
            )
            out[c, :] = (full + c_three[...]).astype(jnp.bfloat16)

    return pl.pallas_call(
        body,
        grid=(queries // block,),
        in_specs=[
            pl.BlockSpec((2, block), lambda i: (0, i)),
            whole(2, trunk),
            whole(1, trunk),
            whole(trunk, trunk),
            whole(1, trunk),
            whole(trunk, basis),
            whole(1, basis),
        ],
        out_specs=[
            pl.BlockSpec((block, basis), lambda i: (i, 0)),
            pl.BlockSpec((block, trunk), lambda i: (i, 0)),
            pl.BlockSpec((block, trunk), lambda i: (i, 0)),
        ],
        out_shape=[
            jax.ShapeDtypeStruct((queries, basis), jnp.bfloat16),
            jax.ShapeDtypeStruct((queries, trunk), jnp.float32),
            jax.ShapeDtypeStruct((queries, trunk), jnp.float32),
        ],
        cost_estimate=pl.CostEstimate(flops=4 * queries * trunk * basis, bytes_accessed=4_000_000, transcendentals=2 * queries * trunk),
        compiler_params=pltpu.CompilerParams(vmem_limit_bytes=60 * 2**20),
        name="trunk_forward",
    )(query_index, v_one, c_one[None], v_two, c_two[None], v_three, c_three[None])


def misfit_of(hidden_all, w_two_all, b_two, basis, targets, inv_scale, grad_scale):
    n = len(hidden_all)
    funcs, queries = targets.shape
    width = basis.shape[1]
    block = BLOCK

    def body(*refs):
        hidden, w_two = refs[:n], refs[n : 2 * n]
        b_two, basis, targets, coeffs, misfit_b, squares, grad = refs[2 * n :]

        @pl.when(pl.program_id(0) == 0)
        def _():
            total = b_two[...]
            for h, w in zip(hidden, w_two):
                total = total + jnp.dot(h[...], w[...], preferred_element_type=jnp.float32)
            coeffs[...] = total.astype(jnp.bfloat16)
            squares[...] = jnp.zeros_like(squares)
            grad[...] = jnp.zeros_like(grad)

        misfit = contract_cols(coeffs[...], basis[...]) * inv_scale - targets[...].astype(jnp.float32)
        total = jnp.sum(misfit * misfit, axis=0, keepdims=True)
        for at in range(0, block, width):
            squares[...] += total[:, at : at + width]
        scaled_b = (misfit * grad_scale).astype(jnp.bfloat16)
        misfit_b[...] = scaled_b
        grad[...] += jnp.dot(scaled_b, basis[...], preferred_element_type=jnp.float32) * inv_scale

    return pl.pallas_call(
        body,
        grid=(queries // block,),
        in_specs=[whole(*h.shape) for h in hidden_all]
        + [whole(*w.shape) for w in w_two_all]
        + [
            whole(1, width),
            pl.BlockSpec((block, width), lambda i: (i, 0)),
            pl.BlockSpec((funcs, block), lambda i: (0, i)),
        ],
        out_specs=[
            whole(funcs, width),
            pl.BlockSpec((funcs, block), lambda i: (0, i)),
            whole(1, width),
            whole(funcs, width),
        ],
        out_shape=[
            jax.ShapeDtypeStruct((funcs, width), jnp.bfloat16),
            jax.ShapeDtypeStruct((funcs, queries), jnp.bfloat16),
            jax.ShapeDtypeStruct((1, width), jnp.float32),
            jax.ShapeDtypeStruct((funcs, width), jnp.float32),
        ],
        cost_estimate=pl.CostEstimate(flops=5 * funcs * queries * width, bytes_accessed=8_000_000, transcendentals=0),
        compiler_params=pltpu.CompilerParams(vmem_limit_bytes=60 * 2**20),
        name="misfit_of",
    )(*hidden_all, *w_two_all, b_two[None], basis, targets)


def pre_of(ix, pieces, hidden, w_two):
    n = len(pieces)
    rows, basis = pieces[0].shape
    funcs, width = hidden.shape

    def body(ix, *refs):
        hidden, w_two, pre_b, bias, product, grad = refs[n:]
        for k in range(n):
            at = lax.rem(ix[0] + n - k, n) * rows
            grad[pl.ds(pl.multiple_of(at, rows), rows), :] = refs[k][...]
        act = hidden[...]
        pre = contract_cols(grad[...], w_two[...]) * (1.0 - act * act)
        pre_b[...] = pre.astype(jnp.bfloat16)
        bias[...] = jnp.sum(pre, axis=0, keepdims=True)
        product[...] = contract_rows(grad[...], act.astype(jnp.bfloat16))

    return pl.pallas_call(
        body,
        grid_spec=pltpu.PrefetchScalarGridSpec(
            num_scalar_prefetch=1,
            grid=(1,),
            in_specs=[whole(rows, basis)] * n + [whole(funcs, width), whole(width, basis)],
            out_specs=[whole(funcs, width), whole(1, width), whole(basis, width)],
            scratch_shapes=[pltpu.VMEM((funcs, basis), jnp.bfloat16)],
        ),
        out_shape=[
            jax.ShapeDtypeStruct((funcs, width), jnp.bfloat16),
            jax.ShapeDtypeStruct((1, width), jnp.float32),
            jax.ShapeDtypeStruct((basis, width), jnp.float32),
        ],
        cost_estimate=pl.CostEstimate(flops=4 * funcs * basis * width, bytes_accessed=2_000_000, transcendentals=0),
        compiler_params=pltpu.CompilerParams(vmem_limit_bytes=12 * 2**20),
        name="pre_of",
    )(ix.reshape(1), *pieces, hidden, w_two)


def columns_by_y(sensors, iy, nz, ny, width):
    funcs = sensors.shape[0]

    def body(y, *refs):
        for src, dst in zip(refs[:ny], refs[ny:]):
            dst[...] = src[...].T

    def source(k):
        return pl.BlockSpec((funcs, width), lambda z, y: (0, z * ny + lax.rem(y[0] + k, ny)))

    return pl.pallas_call(
        body,
        grid_spec=pltpu.PrefetchScalarGridSpec(
            num_scalar_prefetch=1,
            grid=(nz,),
            in_specs=[source(k) for k in range(ny)],
            out_specs=[pl.BlockSpec((width, funcs), lambda z, y: (z, 0))] * ny,
        ),
        out_shape=[jax.ShapeDtypeStruct((nz * width, funcs), sensors.dtype)] * ny,
        cost_estimate=pl.CostEstimate(flops=8_000_000, bytes_accessed=4 * sensors.size, transcendentals=0),
        compiler_params=pltpu.CompilerParams(vmem_limit_bytes=60 * 2**20),
        name="columns_by_y",
    )(iy.reshape(1), *[sensors] * ny)


def back_kernel(core, index, misfit, coeffs, first_act, second_act, v_two, v_three, mine, give, acc3, acc2, accs, *, inv_scale):
    step = pl.program_id(0)

    @pl.when(step == 0)
    def _():
        acc3[...] = jnp.zeros_like(acc3)
        acc2[...] = jnp.zeros_like(acc2)
        accs[...] = jnp.zeros_like(accs)

    x, y = points_of(index[...])
    first, second = first_act[...], second_act[...]
    first_b, second_b = first.astype(jnp.bfloat16), second.astype(jnp.bfloat16)
    grad = contract_rows(misfit[...], coeffs[...]) * inv_scale
    grad_b = grad.astype(jnp.bfloat16)
    acc3[...] += contract_rows(second_b, grad_b)
    accs[4:5, :] += jnp.sum(grad, axis=0, keepdims=True)
    grad = contract_cols(grad_b, v_three[...]) * (1.0 - second * second)
    grad_b = grad.astype(jnp.bfloat16)
    acc2[...] += contract_rows(first_b, grad_b)
    accs[3:4, :] += jnp.sum(grad, axis=0, keepdims=True)
    grad = contract_cols(grad_b, v_two[...]) * (1.0 - first * first)
    accs[2:3, :] += jnp.sum(grad, axis=0, keepdims=True)
    accs[0:1, :] += jnp.sum(x * grad, axis=0, keepdims=True)
    accs[1:2, :] += jnp.sum(y * grad, axis=0, keepdims=True)

    rows = acc3.shape[0]

    @pl.when(step == pl.num_programs(0) - 1)
    def _():
        mine[rows:, :] = accs[...]
        give[rows:, :] = accs[...]

        @pl.when(core[0] == 0)
        def _():
            mine[:rows, :] = acc3[...]
            give[:rows, :] = acc2[...]

        @pl.when(core[0] != 0)
        def _():
            mine[:rows, :] = acc2[...]
            give[:rows, :] = acc3[...]


def trunk_backward(core, query_index, misfit_b, coeffs_b, first_act, second_act, v_two, v_three, inv_scale):
    queries = misfit_b.shape[1]
    funcs, basis = coeffs_b.shape
    trunk = v_two.shape[0]
    block = BLOCK

    out = jax.ShapeDtypeStruct((trunk + 8, basis), jnp.float32)
    return pl.pallas_call(
        functools.partial(back_kernel, inv_scale=inv_scale),
        grid_spec=pltpu.PrefetchScalarGridSpec(
            num_scalar_prefetch=1,
            grid=(queries // block,),
            in_specs=[
                pl.BlockSpec((2, block), lambda i, core: (0, i)),
                pl.BlockSpec((funcs, block), lambda i, core: (0, i)),
                whole(funcs, basis),
                pl.BlockSpec((block, trunk), lambda i, core: (i, 0)),
                pl.BlockSpec((block, trunk), lambda i, core: (i, 0)),
                whole(trunk, trunk),
                whole(trunk, basis),
            ],
            out_specs=[whole(trunk + 8, basis), whole(trunk + 8, basis)],
            scratch_shapes=[
                pltpu.VMEM((trunk, basis), jnp.float32),
                pltpu.VMEM((trunk, trunk), jnp.float32),
                pltpu.VMEM((8, basis), jnp.float32),
            ],
        ),
        out_shape=[out, out],
        cost_estimate=pl.CostEstimate(flops=12 * queries * trunk * basis, bytes_accessed=8_000_000, transcendentals=2 * queries * trunk),
        compiler_params=pltpu.CompilerParams(vmem_limit_bytes=60 * 2**20),
        name="trunk_backward",
    )(core.reshape(1), query_index, misfit_b, coeffs_b, first_act, second_act, v_two, v_three)


def scaled(x, axes=None):
    top = jnp.max(jnp.abs(x), axis=axes, keepdims=True)
    e = jnp.clip(jnp.floor(jnp.log2(jnp.maximum(top, 1e-30))), -100.0, 127.0) - 14.0
    return x * jnp.exp2(-e), e


def summed_in_pairs(x, axis):
    n, k = lax.axis_size(axis), 1
    while k < n:
        pair = k | k >> 1 if 2 * k == n else k
        x = x + lax.ppermute(x, axis, [(i, i ^ pair) for i in range(n)])
        k *= 2
    return x


def with_tail(out, j, big_e, piece, piece_e):
    rows, w = out.shape[1] - 8, out.shape[2]
    out[j, rows:, :] = jnp.zeros((8, w), jnp.float32)
    out[j, rows : rows + 1, : piece.shape[1]] = piece
    out[j, rows + 1 : rows + 2, :] = jnp.broadcast_to(big_e, (1, w))
    out[j, rows + 2 : rows + 3, :] = jnp.broadcast_to(piece_e, (1, w))


def plane_messages(mine, got, b_two, squares, n):
    w = mine.shape[1]
    rows = mine.shape[0] - 8
    per = n // 8
    k = w // per

    def body(mine, got, b_two, squares, out):
        big, big_e = scaled(mine[:rows, :] + got[:rows, :])
        row = lax.broadcasted_iota(jnp.int32, (8, w), 0)
        small = mine[rows:, :] + got[rows:, :]
        small = jnp.where(row == 5, b_two[...], jnp.where(row == 6, squares[...], small))
        small, small_e = scaled(small, 1)
        out[:, : rows // n, :] = big.reshape(n, rows // n, w)
        for j in range(n):
            i, at = j // per, j % per * k
            with_tail(out, j, big_e, small[i : i + 1, at : at + k], small_e[i : i + 1])

    out = pl.pallas_call(
        body,
        out_shape=jax.ShapeDtypeStruct((n, rows // n + 8, w), jnp.float32),
        compiler_params=pltpu.CompilerParams(vmem_limit_bytes=12 * 2**20),
        name="plane_messages",
    )(mine, got, b_two, squares)
    return out.astype(jnp.float16)


def plane_total(got):
    n, rows, w = got.shape[0], got.shape[1] - 8, got.shape[2]

    def body(got, out):
        def total(lo, hi, e):
            x = got[0, lo:hi, :] * jnp.exp2(got[0, e : e + 1, :])
            for j in range(1, n):
                x = x + got[j, lo:hi, :] * jnp.exp2(got[j, e : e + 1, :])
            return x

        out[:rows, :] = total(0, rows, rows + 1)
        out[rows:, :] = jnp.zeros((8, w), jnp.float32)
        out[rows : rows + 1, :] = total(rows, rows + 1, rows + 2)

    return pl.pallas_call(
        body,
        out_shape=jax.ShapeDtypeStruct((rows + 8, w), jnp.float32),
        compiler_params=pltpu.CompilerParams(vmem_limit_bytes=12 * 2**20),
        name="plane_total",
    )(got)


def total_message(both, side):
    rows, w = both.shape[0] - 8, both.shape[1]

    def body(both, out):
        big, big_e = scaled(both[:rows, :])
        small, small_e = scaled(both[rows : rows + 1, :side])
        out[0, :rows, :] = big
        with_tail(out, 0, big_e, small, small_e)

    out = pl.pallas_call(
        body,
        out_shape=jax.ShapeDtypeStruct((1, rows + 8, w), jnp.float32),
        compiler_params=pltpu.CompilerParams(vmem_limit_bytes=12 * 2**20),
        name="total_message",
    )(both)
    return out[0].astype(jnp.float16)


def z_messages(core, w_one_part, got, w_two_part, b_one_row):
    nz, _, rows, w = w_one_part.shape
    m = w_two_part.shape[1]

    def body(core, part, got, two, bias, out):
        one, one_e = scaled(part[:, 0] + got[...])
        two, two_e = scaled(two[...])
        bias, bias_e = scaled(bias[...])
        out[:, :rows, :] = one
        out[:, rows : rows + m, :] = two
        for j in range(nz):
            out[j, rows + m :, :] = jnp.zeros((8, w), jnp.float32)
            for i, row in enumerate((bias, bias_e, two_e, one_e)):
                out[j, rows + m + i : rows + m + i + 1, :] = jnp.broadcast_to(row.reshape(1, -1), (1, w))

    out = pl.pallas_call(
        body,
        grid_spec=pltpu.PrefetchScalarGridSpec(
            num_scalar_prefetch=1,
            grid=(1,),
            in_specs=[
                pl.BlockSpec((nz, 1, rows, w), lambda i, core: (0, core[0], 0, 0)),
                pl.BlockSpec((nz, rows, w), lambda i, core: (0, 0, 0)),
                pl.BlockSpec((nz, m, w), lambda i, core: (0, 0, 0)),
                pl.BlockSpec((1, w), lambda i, core: (0, 0)),
            ],
            out_specs=pl.BlockSpec((nz, rows + m + 8, w), lambda i, core: (0, 0, 0)),
        ),
        out_shape=jax.ShapeDtypeStruct((nz, rows + m + 8, w), jnp.float32),
        compiler_params=pltpu.CompilerParams(vmem_limit_bytes=12 * 2**20),
        name="z_messages",
    )(core.reshape(1), w_one_part, got, w_two_part, b_one_row)
    return out.astype(jnp.float16)


def finished(place, got, other, side):
    ny = len(got)
    nx, rows, w = got[0].shape[0], got[0].shape[1] - 8, got[0].shape[2]
    n = ny * nx
    per = n // 8

    def body(place, *refs):
        got, other = refs[:ny], refs[ny : 2 * ny]
        one, two, v_one, c_one, c_two, c_three, b_two, loss, small, more = refs[2 * ny :]

        def put(zero, last):
            for q in range(n):
                at = lax.rem(place[1] + ny - q // nx, ny) * nx + lax.rem(place[2] + nx - q % nx, nx)
                into = pl.ds(pl.multiple_of(at * rows, rows), rows)
                for refs, out, part in ((zero, one, small), (last, two, more)):
                    x, i = refs[q // nx], q % nx
                    out[into, :] = x[i, :rows, :] * jnp.exp2(x[i, rows + 1 : rows + 2, :])
                    part[pl.ds(at, 1), :] = x[i, rows : rows + 1, :side] * jnp.exp2(
                        x[i, rows + 2 : rows + 3, :side]
                    )

        @pl.when(place[0] == 0)
        def _():
            put(got, other)

        @pl.when(place[0] != 0)
        def _():
            put(other, got)

        total = jnp.zeros((1, 1), jnp.float32)
        for p in range(per):
            at = slice(p * side, (p + 1) * side)
            for i, (out, j) in enumerate(((v_one, 0), (v_one, 1), (c_one, 0), (c_two, 0), (c_three, 0))):
                out[j : j + 1, at] = small[i * per + p : i * per + p + 1, :]
            k = 5 * per + p
            b_two[:, at] = small[k : k + 1, :] + more[k : k + 1, :]
            k = 6 * per + p
            total = total + jnp.sum(small[k : k + 1, :] + more[k : k + 1, :], axis=1, keepdims=True)
        loss[...] = total

    shapes = [(n * rows, w), (n * rows, w), (2, w)] + [(1, w)] * 4 + [(1, 1)]
    return pl.pallas_call(
        body,
        grid_spec=pltpu.PrefetchScalarGridSpec(
            num_scalar_prefetch=1,
            grid=(1,),
            in_specs=[whole(*x.shape) for x in (*got, *other)],
            out_specs=[whole(*shape) for shape in shapes],
            scratch_shapes=[pltpu.VMEM((n, side), jnp.float32)] * 2,
        ),
        out_shape=[jax.ShapeDtypeStruct(shape, jnp.float32) for shape in shapes],
        compiler_params=pltpu.CompilerParams(vmem_limit_bytes=24 * 2**20),
        name="finished",
    )(place, *got, *other)


def z_finished(got, rows):
    nz, all_rows, w = got.shape
    m = all_rows - rows - 8

    def body(got, one, two, bias):
        def part(lo, hi, e):
            total = got[0, lo:hi, :] * jnp.exp2(got[0, e : e + 1, :])
            for j in range(1, nz):
                total = total + got[j, lo:hi, :] * jnp.exp2(got[j, e : e + 1, :])
            return total

        k = rows + m
        one[...] = part(0, rows, k + 3)
        two[...] = part(rows, k, k + 2)
        bias[...] = part(k, k + 1, k + 1)

    return pl.pallas_call(
        body,
        out_shape=[jax.ShapeDtypeStruct(shape, jnp.float32) for shape in ((rows, w), (m, w), (1, w))],
        compiler_params=pltpu.CompilerParams(vmem_limit_bytes=12 * 2**20),
        name="z_finished",
    )(got)


def sum_of_all(mine, give, b_two, squares):
    w = mine.shape[1]
    ny, nx = lax.axis_size("y"), lax.axis_size("query")
    n = ny * nx
    side = 8 * w // n
    got = other_core(give)

    got = exchanged(plane_messages(mine, got, b_two, squares, n), ("y", "query"))
    both = plane_total(got.astype(jnp.float32))
    both = summed_in_pairs(both, "z")
    got = total_message(both, side)
    got = jnp.stack([got] + [shift(got, "query", k) for k in range(1, nx)])
    pieces = [got] + [shift(got, "y", k) for k in range(1, ny)]
    others = [other_core(p) for p in pieces]
    place = jnp.stack([lax.axis_index(a) for a in ("c", "y", "query")])
    return finished(
        place,
        [p.astype(jnp.float32) for p in pieces],
        [p.astype(jnp.float32) for p in others],
        side,
    )


def local(
    sensors,
    query_index,
    targets,
    w_one,
    b_one,
    w_two,
    b_two,
    v_one,
    c_one,
    v_two,
    c_two,
    v_three,
    c_three,
):
    funcs, sensor_count = sensors.shape
    hidden_count, basis_count = w_two.shape
    query_rows = query_index.shape[1]
    nz, ny, nc, nx = (lax.axis_size(a) for a in ALL)
    count_all = funcs * nz * ny * nc * query_rows * nx
    grad_scale = 64.0 / math.sqrt(count_all)
    inv_scale = 1.0 / math.sqrt(basis_count)

    w_two_all = [w_two] + [shift(w_two, "query", k) for k in range(1, nx)]
    hidden = jnp.tanh(jnp.dot(sensors, w_one, preferred_element_type=jnp.float32) + b_one)
    hidden_b = hidden.astype(jnp.bfloat16)
    hidden_all = [hidden_b] + [shift(hidden_b, "query", k) for k in range(1, nx)]
    basis, first_act, second_act = trunk_forward(
        query_index, v_one, c_one, v_two, c_two, v_three, c_three
    )

    rows_own = sensor_count // (nz * ny * nc)
    iy, ic = lax.axis_index("y"), lax.axis_index("c")
    sensors_late, _ = lax.optimization_barrier((sensors, hidden_b))
    sens_y = columns_by_y(sensors_late, iy, nz, ny, nc * rows_own)
    sens_y = [sens_y[0]] + [shift(sens_y[k], "y", k) for k in range(1, ny)]

    coeffs_b, misfit_b, squares, grad_part = misfit_of(
        hidden_all, w_two_all, b_two, basis, targets, inv_scale, grad_scale
    )
    grad_own = exchanged(grad_part.reshape(nx, -1, basis_count), "query")
    grad_own = jnp.sum(grad_own, axis=0)
    b_two_part = jnp.sum(grad_own, axis=0, keepdims=True)
    grad_own_b = grad_own.astype(jnp.bfloat16)
    grad_pieces = [grad_own_b] + [shift(grad_own_b, "query", k) for k in range(1, nx)]

    mine, give = trunk_backward(ic, query_index, misfit_b, coeffs_b, first_act, second_act, v_two, v_three, inv_scale)
    totals = sum_of_all(mine, give, b_two_part, squares)
    g_v_three, g_v_two, g_v_one, g_c_one, g_c_two, g_c_three, g_b_two, loss = totals

    grad_pre_b, b_one_part, w_two_part = pre_of(
        lax.axis_index("query"), grad_pieces, hidden, w_two
    )

    pre_y = [grad_pre_b] + [shift(grad_pre_b, "y", k) for k in range(1, ny)]

    w_two_part = w_two_part.reshape(nz, ny, nc, -1, hidden_count)
    b_one_rows = jnp.pad(b_one_part, ((0, 7), (0, 0)))

    def with_bias(rows, n):
        rows = rows.reshape(n, -1, hidden_count)
        bias = jnp.broadcast_to(b_one_rows, (n, 8, hidden_count))
        return jnp.concatenate([rows, bias], axis=1)

    both = scattered_sum(with_bias(w_two_part.transpose(2, 0, 1, 3, 4), nc), "c")
    w_two_part, b_one_rows = both[:-8].reshape(nz, ny, -1, hidden_count), both[-8:]
    both = scattered_sum(with_bias(w_two_part.transpose(1, 0, 2, 3), ny), "y")
    w_two_part, b_one_row = both[:-8].reshape(nz, -1, hidden_count), both[-8:-7]

    w_one_part = jnp.dot(sens_y[0], pre_y[0], preferred_element_type=jnp.float32)
    for k in range(1, ny):
        w_one_part = w_one_part + jnp.dot(
            sens_y[k], pre_y[k], preferred_element_type=jnp.float32
        )
    w_one_part = w_one_part.reshape(nz, nc, rows_own, hidden_count)
    got = other_core(lax.dynamic_index_in_dim(w_one_part, 1 - ic, 1, False))
    sent = z_messages(ic, w_one_part, got, w_two_part, b_one_row)
    got = exchanged(sent, "z")
    grad_w_one, grad_w_two, grad_b_one = z_finished(got.astype(jnp.float32), rows_own)
    return (
        loss[0, 0] / count_all,
        grad_w_one,
        grad_b_one[0],
        grad_w_two.T,
        g_b_two[0],
        g_v_one,
        g_c_one[0],
        g_v_two,
        g_c_two[0],
        g_v_three,
        g_c_three[0],
    )


def solution(mesh):
    torus = Mesh(mesh.devices.reshape(8, 4, 2, mesh.shape["query"]), ALL)
    return jax.shard_map(
        local,
        mesh=torus,
        in_specs=(
            P(DP, None),
            P(None, "query"),
            P(DP, "query"),
            P(None, "query"),
            P("query"),
            P("query", None),
            P(),
            P(),
            P(),
            P(),
            P(),
            P(),
            P(),
        ),
        out_specs=(
            P(),
            P(DP, "query"),
            P("query"),
            P("query", DP),
            P(),
            P(),
            P(),
            P(),
            P(),
            P(),
            P(),
        ),
        check_vma=False,
    )
```

```python
import functools
import math

import jax
import jax.numpy as jnp
from jax import lax
from jax.experimental import pallas as pl
from jax.experimental.pallas import tpu as pltpu
from jax.sharding import Mesh
from jax.sharding import PartitionSpec as P


GRID = 128
BLOCK = 1024
CUT = 1024
DP = ("z", "y", "c")
ALL = ("z", "y", "c", "query")


def shift(x, axis, k):
    n = lax.axis_size(axis)
    return lax.ppermute(x, axis, [(i, (i + k) % n) for i in range(n)])


def part(x, i):
    return lax.dynamic_index_in_dim(x, i, 0, False)


def scattered_sum(chunks, axis):
    n, i = lax.axis_size(axis), lax.axis_index(axis)
    arrived = [shift(part(chunks, (i + k) % n), axis, k) for k in range(1, n)]
    total = part(chunks, i)
    for a in arrived:
        total = total + a
    return total


def exchanged(x, axis):
    return lax.all_to_all(x, axis, 0, 0, tiled=True)


def other_core(x):
    return lax.ppermute(x, "c", [(0, 1), (1, 0)])


def contract_rows(left, right, precision=None):
    return lax.dot_general(
        left,
        right,
        (((0,), (0,)), ((), ())),
        precision=precision,
        preferred_element_type=jnp.float32,
    )


def contract_cols(left, right, precision=None):
    return lax.dot_general(
        left,
        right,
        (((1,), (1,)), ((), ())),
        precision=precision,
        preferred_element_type=jnp.float32,
    )


def points_of(index):
    coords = index.astype(jnp.float32) / (GRID - 1)
    columns = jnp.concatenate([coords, jnp.zeros((6, coords.shape[1]), jnp.float32)]).T
    return columns[:, 0:1], columns[:, 1:2]


def whole(*shape):
    return pl.BlockSpec(shape, lambda i, *_: (0,) * len(shape))


def trunk_forward(query_index, v_one, c_one, v_two, c_two, v_three, c_three):
    queries = query_index.shape[1]
    trunk, basis = v_three.shape
    block = BLOCK

    def body(index, v_one, c_one, v_two, c_two, v_three, c_three, out, first_out, second_out):
        x, y = points_of(index[...])
        cuts = [slice(at, at + CUT) for at in range(0, block, CUT)]
        firsts = [
            jnp.tanh(x[c] * v_one[0:1, :] + y[c] * v_one[1:2, :] + c_one[...]) for c in cuts
        ]
        seconds = [
            jnp.dot(first.astype(jnp.bfloat16), v_two[...], preferred_element_type=jnp.float32)
            for first in firsts
        ]
        seconds = [jnp.tanh(second + c_two[...]) for second in seconds]
        for c, first, second in zip(cuts, firsts, seconds):
            first_out[c, :] = first
            second_out[c, :] = second
            full = jnp.dot(
                second.astype(jnp.bfloat16), v_three[...], preferred_element_type=jnp.float32
            )
            out[c, :] = (full + c_three[...]).astype(jnp.bfloat16)

    return pl.pallas_call(
        body,
        grid=(queries // block,),
        in_specs=[
            pl.BlockSpec((2, block), lambda i: (0, i)),
            whole(2, trunk),
            whole(1, trunk),
            whole(trunk, trunk),
            whole(1, trunk),
            whole(trunk, basis),
            whole(1, basis),
        ],
        out_specs=[
            pl.BlockSpec((block, basis), lambda i: (i, 0)),
            pl.BlockSpec((block, trunk), lambda i: (i, 0)),
            pl.BlockSpec((block, trunk), lambda i: (i, 0)),
        ],
        out_shape=[
            jax.ShapeDtypeStruct((queries, basis), jnp.bfloat16),
            jax.ShapeDtypeStruct((queries, trunk), jnp.float32),
            jax.ShapeDtypeStruct((queries, trunk), jnp.float32),
        ],
        cost_estimate=pl.CostEstimate(flops=4 * queries * trunk * basis, bytes_accessed=4_000_000, transcendentals=2 * queries * trunk),
        compiler_params=pltpu.CompilerParams(vmem_limit_bytes=60 * 2**20),
        name="trunk_forward",
    )(query_index, v_one, c_one[None], v_two, c_two[None], v_three, c_three[None])


def misfit_of(hidden_all, w_two_all, b_two, basis, targets, inv_scale, grad_scale):
    n = len(hidden_all)
    funcs, queries = targets.shape
    width = basis.shape[1]
    block = BLOCK

    def body(*refs):
        hidden, w_two = refs[:n], refs[n : 2 * n]
        b_two, basis, targets, coeffs, misfit_b, squares, grad = refs[2 * n :]

        @pl.when(pl.program_id(0) == 0)
        def _():
            total = b_two[...]
            for h, w in zip(hidden, w_two):
                total = total + jnp.dot(h[...], w[...], preferred_element_type=jnp.float32)
            coeffs[...] = total.astype(jnp.bfloat16)
            squares[...] = jnp.zeros_like(squares)
            grad[...] = jnp.zeros_like(grad)

        misfit = contract_cols(coeffs[...], basis[...]) * inv_scale - targets[...].astype(jnp.float32)
        total = jnp.sum(misfit * misfit, axis=0, keepdims=True)
        for at in range(0, block, width):
            squares[...] += total[:, at : at + width]
        scaled_b = (misfit * grad_scale).astype(jnp.bfloat16)
        misfit_b[...] = scaled_b
        grad[...] += jnp.dot(scaled_b, basis[...], preferred_element_type=jnp.float32) * inv_scale

    return pl.pallas_call(
        body,
        grid=(queries // block,),
        in_specs=[whole(*h.shape) for h in hidden_all]
        + [whole(*w.shape) for w in w_two_all]
        + [
            whole(1, width),
            pl.BlockSpec((block, width), lambda i: (i, 0)),
            pl.BlockSpec((funcs, block), lambda i: (0, i)),
        ],
        out_specs=[
            whole(funcs, width),
            pl.BlockSpec((funcs, block), lambda i: (0, i)),
            whole(1, width),
            whole(funcs, width),
        ],
        out_shape=[
            jax.ShapeDtypeStruct((funcs, width), jnp.bfloat16),
            jax.ShapeDtypeStruct((funcs, queries), jnp.bfloat16),
            jax.ShapeDtypeStruct((1, width), jnp.float32),
            jax.ShapeDtypeStruct((funcs, width), jnp.float32),
        ],
        cost_estimate=pl.CostEstimate(flops=5 * funcs * queries * width, bytes_accessed=8_000_000, transcendentals=0),
        compiler_params=pltpu.CompilerParams(vmem_limit_bytes=60 * 2**20),
        name="misfit_of",
    )(*hidden_all, *w_two_all, b_two[None], basis, targets)


def pre_of(ix, pieces, hidden, w_two):
    n = len(pieces)
    rows, basis = pieces[0].shape
    funcs, width = hidden.shape

    def body(ix, *refs):
        hidden, w_two, pre_b, bias, product, grad = refs[n:]
        for k in range(n):
            at = lax.rem(ix[0] + n - k, n) * rows
            grad[pl.ds(pl.multiple_of(at, rows), rows), :] = refs[k][...]
        act = hidden[...]
        pre = contract_cols(grad[...], w_two[...]) * (1.0 - act * act)
        pre_b[...] = pre.astype(jnp.bfloat16)
        bias[...] = jnp.sum(pre, axis=0, keepdims=True)
        product[...] = contract_rows(grad[...], act.astype(jnp.bfloat16))

    return pl.pallas_call(
        body,
        grid_spec=pltpu.PrefetchScalarGridSpec(
            num_scalar_prefetch=1,
            grid=(1,),
            in_specs=[whole(rows, basis)] * n + [whole(funcs, width), whole(width, basis)],
            out_specs=[whole(funcs, width), whole(1, width), whole(basis, width)],
            scratch_shapes=[pltpu.VMEM((funcs, basis), jnp.bfloat16)],
        ),
        out_shape=[
            jax.ShapeDtypeStruct((funcs, width), jnp.bfloat16),
            jax.ShapeDtypeStruct((1, width), jnp.float32),
            jax.ShapeDtypeStruct((basis, width), jnp.float32),
        ],
        cost_estimate=pl.CostEstimate(flops=4 * funcs * basis * width, bytes_accessed=2_000_000, transcendentals=0),
        compiler_params=pltpu.CompilerParams(vmem_limit_bytes=12 * 2**20),
        name="pre_of",
    )(ix.reshape(1), *pieces, hidden, w_two)


def columns_by_y(sensors, iy, nz, ny, width):
    funcs = sensors.shape[0]

    def body(y, src, *out):
        for k, dst in enumerate(out):
            at = lax.rem(y[0] + k, ny) * width
            dst[...] = src[:, pl.ds(pl.multiple_of(at, width), width)].T

    return pl.pallas_call(
        body,
        grid_spec=pltpu.PrefetchScalarGridSpec(
            num_scalar_prefetch=1,
            grid=(nz,),
            in_specs=[pl.BlockSpec((funcs, ny * width), lambda z, y: (0, z))],
            out_specs=[pl.BlockSpec((width, funcs), lambda z, y: (z, 0))] * ny,
        ),
        out_shape=[jax.ShapeDtypeStruct((nz * width, funcs), sensors.dtype)] * ny,
        cost_estimate=pl.CostEstimate(flops=8_000_000, bytes_accessed=4 * sensors.size, transcendentals=0),
        compiler_params=pltpu.CompilerParams(vmem_limit_bytes=60 * 2**20),
        name="columns_by_y",
    )(iy.reshape(1), sensors)


def back_kernel(core, index, misfit, coeffs, first_act, second_act, v_two, v_three, mine, give, acc3, acc2, accs, *, inv_scale):
    step = pl.program_id(0)

    @pl.when(step == 0)
    def _():
        acc3[...] = jnp.zeros_like(acc3)
        acc2[...] = jnp.zeros_like(acc2)
        accs[...] = jnp.zeros_like(accs)

    x, y = points_of(index[...])
    first, second = first_act[...], second_act[...]
    first_b, second_b = first.astype(jnp.bfloat16), second.astype(jnp.bfloat16)
    grad = contract_rows(misfit[...], coeffs[...]) * inv_scale
    grad_b = grad.astype(jnp.bfloat16)
    acc3[...] += contract_rows(second_b, grad_b)
    accs[4:5, :] += jnp.sum(grad, axis=0, keepdims=True)
    grad = contract_cols(grad_b, v_three[...]) * (1.0 - second * second)
    grad_b = grad.astype(jnp.bfloat16)
    acc2[...] += contract_rows(first_b, grad_b)
    accs[3:4, :] += jnp.sum(grad, axis=0, keepdims=True)
    grad = contract_cols(grad_b, v_two[...]) * (1.0 - first * first)
    accs[2:3, :] += jnp.sum(grad, axis=0, keepdims=True)
    accs[0:1, :] += jnp.sum(x * grad, axis=0, keepdims=True)
    accs[1:2, :] += jnp.sum(y * grad, axis=0, keepdims=True)

    rows = acc3.shape[0]

    @pl.when(step == pl.num_programs(0) - 1)
    def _():
        mine[rows:, :] = accs[...]
        give[rows:, :] = accs[...]

        @pl.when(core[0] == 0)
        def _():
            mine[:rows, :] = acc3[...]
            give[:rows, :] = acc2[...]

        @pl.when(core[0] != 0)
        def _():
            mine[:rows, :] = acc2[...]
            give[:rows, :] = acc3[...]


def trunk_backward(core, query_index, misfit_b, coeffs_b, first_act, second_act, v_two, v_three, inv_scale):
    queries = misfit_b.shape[1]
    funcs, basis = coeffs_b.shape
    trunk = v_two.shape[0]
    block = BLOCK

    out = jax.ShapeDtypeStruct((trunk + 8, basis), jnp.float32)
    return pl.pallas_call(
        functools.partial(back_kernel, inv_scale=inv_scale),
        grid_spec=pltpu.PrefetchScalarGridSpec(
            num_scalar_prefetch=1,
            grid=(queries // block,),
            in_specs=[
                pl.BlockSpec((2, block), lambda i, core: (0, i)),
                pl.BlockSpec((funcs, block), lambda i, core: (0, i)),
                whole(funcs, basis),
                pl.BlockSpec((block, trunk), lambda i, core: (i, 0)),
                pl.BlockSpec((block, trunk), lambda i, core: (i, 0)),
                whole(trunk, trunk),
                whole(trunk, basis),
            ],
            out_specs=[whole(trunk + 8, basis), whole(trunk + 8, basis)],
            scratch_shapes=[
                pltpu.VMEM((trunk, basis), jnp.float32),
                pltpu.VMEM((trunk, trunk), jnp.float32),
                pltpu.VMEM((8, basis), jnp.float32),
            ],
        ),
        out_shape=[out, out],
        cost_estimate=pl.CostEstimate(flops=12 * queries * trunk * basis, bytes_accessed=8_000_000, transcendentals=2 * queries * trunk),
        compiler_params=pltpu.CompilerParams(vmem_limit_bytes=60 * 2**20),
        name="trunk_backward",
    )(core.reshape(1), query_index, misfit_b, coeffs_b, first_act, second_act, v_two, v_three)


def scaled(x, axes=None):
    top = jnp.max(jnp.abs(x), axis=axes, keepdims=True)
    e = jnp.clip(jnp.floor(jnp.log2(jnp.maximum(top, 1e-30))), -100.0, 127.0) - 14.0
    return x * jnp.exp2(-e), e


def summed_in_pairs(x, axis):
    n, k = lax.axis_size(axis), 1
    while k < n:
        pair = k | k >> 1 if 2 * k == n else k
        x = x + lax.ppermute(x, axis, [(i, i ^ pair) for i in range(n)])
        k *= 2
    return x


def with_tail(out, j, big_e, piece, piece_e):
    rows, w = out.shape[1] - 8, out.shape[2]
    out[j, rows:, :] = jnp.zeros((8, w), jnp.float32)
    out[j, rows : rows + 1, : piece.shape[1]] = piece
    out[j, rows + 1 : rows + 2, :] = jnp.broadcast_to(big_e, (1, w))
    out[j, rows + 2 : rows + 3, :] = jnp.broadcast_to(piece_e, (1, w))


def plane_messages(mine, got, b_two, squares, n):
    w = mine.shape[1]
    rows = mine.shape[0] - 8
    per = n // 8
    k = w // per

    def body(mine, got, b_two, squares, out):
        big, big_e = scaled(mine[:rows, :] + got[:rows, :])
        row = lax.broadcasted_iota(jnp.int32, (8, w), 0)
        small = mine[rows:, :] + got[rows:, :]
        small = jnp.where(row == 5, b_two[...], jnp.where(row == 6, squares[...], small))
        small, small_e = scaled(small, 1)
        out[:, : rows // n, :] = big.reshape(n, rows // n, w)
        for j in range(n):
            i, at = j // per, j % per * k
            with_tail(out, j, big_e, small[i : i + 1, at : at + k], small_e[i : i + 1])

    out = pl.pallas_call(
        body,
        out_shape=jax.ShapeDtypeStruct((n, rows // n + 8, w), jnp.float32),
        compiler_params=pltpu.CompilerParams(vmem_limit_bytes=12 * 2**20),
        name="plane_messages",
    )(mine, got, b_two, squares)
    return out.astype(jnp.float16)


def plane_total(got):
    n, rows, w = got.shape[0], got.shape[1] - 8, got.shape[2]

    def body(got, out):
        def total(lo, hi, e):
            x = got[0, lo:hi, :] * jnp.exp2(got[0, e : e + 1, :])
            for j in range(1, n):
                x = x + got[j, lo:hi, :] * jnp.exp2(got[j, e : e + 1, :])
            return x

        out[:rows, :] = total(0, rows, rows + 1)
        out[rows:, :] = jnp.zeros((8, w), jnp.float32)
        out[rows : rows + 1, :] = total(rows, rows + 1, rows + 2)

    return pl.pallas_call(
        body,
        out_shape=jax.ShapeDtypeStruct((rows + 8, w), jnp.float32),
        compiler_params=pltpu.CompilerParams(vmem_limit_bytes=12 * 2**20),
        name="plane_total",
    )(got)


def total_message(both, side):
    rows, w = both.shape[0] - 8, both.shape[1]

    def body(both, out):
        big, big_e = scaled(both[:rows, :])
        small, small_e = scaled(both[rows : rows + 1, :side])
        out[0, :rows, :] = big
        with_tail(out, 0, big_e, small, small_e)

    out = pl.pallas_call(
        body,
        out_shape=jax.ShapeDtypeStruct((1, rows + 8, w), jnp.float32),
        compiler_params=pltpu.CompilerParams(vmem_limit_bytes=12 * 2**20),
        name="total_message",
    )(both)
    return out[0].astype(jnp.float16)


def z_messages(core, w_one_part, got, w_two_part, b_one_row):
    nz, _, rows, w = w_one_part.shape
    m = w_two_part.shape[1]

    def body(core, part, got, two, bias, out):
        one, one_e = scaled(part[:, 0] + got[...])
        two, two_e = scaled(two[...])
        bias, bias_e = scaled(bias[...])
        out[:, :rows, :] = one
        out[:, rows : rows + m, :] = two
        for j in range(nz):
            out[j, rows + m :, :] = jnp.zeros((8, w), jnp.float32)
            for i, row in enumerate((bias, bias_e, two_e, one_e)):
                out[j, rows + m + i : rows + m + i + 1, :] = jnp.broadcast_to(row.reshape(1, -1), (1, w))

    out = pl.pallas_call(
        body,
        grid_spec=pltpu.PrefetchScalarGridSpec(
            num_scalar_prefetch=1,
            grid=(1,),
            in_specs=[
                pl.BlockSpec((nz, 1, rows, w), lambda i, core: (0, core[0], 0, 0)),
                pl.BlockSpec((nz, rows, w), lambda i, core: (0, 0, 0)),
                pl.BlockSpec((nz, m, w), lambda i, core: (0, 0, 0)),
                pl.BlockSpec((1, w), lambda i, core: (0, 0)),
            ],
            out_specs=pl.BlockSpec((nz, rows + m + 8, w), lambda i, core: (0, 0, 0)),
        ),
        out_shape=jax.ShapeDtypeStruct((nz, rows + m + 8, w), jnp.float32),
        compiler_params=pltpu.CompilerParams(vmem_limit_bytes=12 * 2**20),
        name="z_messages",
    )(core.reshape(1), w_one_part, got, w_two_part, b_one_row)
    return out.astype(jnp.float16)


def finished(place, got, other, side):
    ny = len(got)
    nx, rows, w = got[0].shape[0], got[0].shape[1] - 8, got[0].shape[2]
    n = ny * nx
    per = n // 8

    def body(place, *refs):
        got, other = refs[:ny], refs[ny : 2 * ny]
        one, two, v_one, c_one, c_two, c_three, b_two, loss, small, more = refs[2 * ny :]

        def put(zero, last):
            for q in range(n):
                at = lax.rem(place[1] + ny - q // nx, ny) * nx + lax.rem(place[2] + nx - q % nx, nx)
                into = pl.ds(pl.multiple_of(at * rows, rows), rows)
                for refs, out, part in ((zero, one, small), (last, two, more)):
                    x, i = refs[q // nx], q % nx
                    out[into, :] = x[i, :rows, :] * jnp.exp2(x[i, rows + 1 : rows + 2, :])
                    part[pl.ds(at, 1), :] = x[i, rows : rows + 1, :side] * jnp.exp2(
                        x[i, rows + 2 : rows + 3, :side]
                    )

        @pl.when(place[0] == 0)
        def _():
            put(got, other)

        @pl.when(place[0] != 0)
        def _():
            put(other, got)

        total = jnp.zeros((1, 1), jnp.float32)
        for p in range(per):
            at = slice(p * side, (p + 1) * side)
            for i, (out, j) in enumerate(((v_one, 0), (v_one, 1), (c_one, 0), (c_two, 0), (c_three, 0))):
                out[j : j + 1, at] = small[i * per + p : i * per + p + 1, :]
            k = 5 * per + p
            b_two[:, at] = small[k : k + 1, :] + more[k : k + 1, :]
            k = 6 * per + p
            total = total + jnp.sum(small[k : k + 1, :] + more[k : k + 1, :], axis=1, keepdims=True)
        loss[...] = total

    shapes = [(n * rows, w), (n * rows, w), (2, w)] + [(1, w)] * 4 + [(1, 1)]
    return pl.pallas_call(
        body,
        grid_spec=pltpu.PrefetchScalarGridSpec(
            num_scalar_prefetch=1,
            grid=(1,),
            in_specs=[whole(*x.shape) for x in (*got, *other)],
            out_specs=[whole(*shape) for shape in shapes],
            scratch_shapes=[pltpu.VMEM((n, side), jnp.float32)] * 2,
        ),
        out_shape=[jax.ShapeDtypeStruct(shape, jnp.float32) for shape in shapes],
        compiler_params=pltpu.CompilerParams(vmem_limit_bytes=24 * 2**20),
        name="finished",
    )(place, *got, *other)


def z_finished(got, rows):
    nz, all_rows, w = got.shape
    m = all_rows - rows - 8

    def body(got, one, two, bias):
        def part(lo, hi, e):
            total = got[0, lo:hi, :] * jnp.exp2(got[0, e : e + 1, :])
            for j in range(1, nz):
                total = total + got[j, lo:hi, :] * jnp.exp2(got[j, e : e + 1, :])
            return total

        k = rows + m
        one[...] = part(0, rows, k + 3)
        two[...] = part(rows, k, k + 2)
        bias[...] = part(k, k + 1, k + 1)

    return pl.pallas_call(
        body,
        out_shape=[jax.ShapeDtypeStruct(shape, jnp.float32) for shape in ((rows, w), (m, w), (1, w))],
        compiler_params=pltpu.CompilerParams(vmem_limit_bytes=12 * 2**20),
        name="z_finished",
    )(got)


def sum_of_all(mine, give, b_two, squares):
    w = mine.shape[1]
    ny, nx = lax.axis_size("y"), lax.axis_size("query")
    n = ny * nx
    side = 8 * w // n
    got = other_core(give)

    got = exchanged(plane_messages(mine, got, b_two, squares, n), ("y", "query"))
    both = plane_total(got.astype(jnp.float32))
    both = summed_in_pairs(both, "z")
    got = total_message(both, side)
    got = jnp.stack([got] + [shift(got, "query", k) for k in range(1, nx)])
    pieces = [got] + [shift(got, "y", k) for k in range(1, ny)]
    others = [other_core(p) for p in pieces]
    place = jnp.stack([lax.axis_index(a) for a in ("c", "y", "query")])
    return finished(
        place,
        [p.astype(jnp.float32) for p in pieces],
        [p.astype(jnp.float32) for p in others],
        side,
    )


def local(
    sensors,
    query_index,
    targets,
    w_one,
    b_one,
    w_two,
    b_two,
    v_one,
    c_one,
    v_two,
    c_two,
    v_three,
    c_three,
):
    funcs, sensor_count = sensors.shape
    hidden_count, basis_count = w_two.shape
    query_rows = query_index.shape[1]
    nz, ny, nc, nx = (lax.axis_size(a) for a in ALL)
    count_all = funcs * nz * ny * nc * query_rows * nx
    grad_scale = 64.0 / math.sqrt(count_all)
    inv_scale = 1.0 / math.sqrt(basis_count)

    w_two_all = [w_two] + [shift(w_two, "query", k) for k in range(1, nx)]
    hidden = jnp.tanh(jnp.dot(sensors, w_one, preferred_element_type=jnp.float32) + b_one)
    hidden_b = hidden.astype(jnp.bfloat16)
    hidden_all = [hidden_b] + [shift(hidden_b, "query", k) for k in range(1, nx)]
    basis, first_act, second_act = trunk_forward(
        query_index, v_one, c_one, v_two, c_two, v_three, c_three
    )

    rows_own = sensor_count // (nz * ny * nc)
    iy, ic = lax.axis_index("y"), lax.axis_index("c")
    sensors_late, _ = lax.optimization_barrier((sensors, hidden_b))
    sens_y = columns_by_y(sensors_late, iy, nz, ny, nc * rows_own)
    sens_y = [sens_y[0]] + [shift(sens_y[k], "y", k) for k in range(1, ny)]

    coeffs_b, misfit_b, squares, grad_part = misfit_of(
        hidden_all, w_two_all, b_two, basis, targets, inv_scale, grad_scale
    )
    grad_own = exchanged(grad_part.reshape(nx, -1, basis_count), "query")
    grad_own = jnp.sum(grad_own, axis=0)
    b_two_part = jnp.sum(grad_own, axis=0, keepdims=True)
    grad_own_b = grad_own.astype(jnp.bfloat16)
    grad_pieces = [grad_own_b] + [shift(grad_own_b, "query", k) for k in range(1, nx)]

    mine, give = trunk_backward(ic, query_index, misfit_b, coeffs_b, first_act, second_act, v_two, v_three, inv_scale)
    totals = sum_of_all(mine, give, b_two_part, squares)
    g_v_three, g_v_two, g_v_one, g_c_one, g_c_two, g_c_three, g_b_two, loss = totals

    grad_pre_b, b_one_part, w_two_part = pre_of(
        lax.axis_index("query"), grad_pieces, hidden, w_two
    )

    pre_y = [grad_pre_b] + [shift(grad_pre_b, "y", k) for k in range(1, ny)]

    w_two_part = w_two_part.reshape(nz, ny, nc, -1, hidden_count)
    b_one_rows = jnp.pad(b_one_part, ((0, 7), (0, 0)))

    def with_bias(rows, n):
        rows = rows.reshape(n, -1, hidden_count)
        bias = jnp.broadcast_to(b_one_rows, (n, 8, hidden_count))
        return jnp.concatenate([rows, bias], axis=1)

    both = scattered_sum(with_bias(w_two_part.transpose(2, 0, 1, 3, 4), nc), "c")
    w_two_part, b_one_rows = both[:-8].reshape(nz, ny, -1, hidden_count), both[-8:]
    both = scattered_sum(with_bias(w_two_part.transpose(1, 0, 2, 3), ny), "y")
    w_two_part, b_one_row = both[:-8].reshape(nz, -1, hidden_count), both[-8:-7]

    w_one_part = jnp.dot(sens_y[0], pre_y[0], preferred_element_type=jnp.float32)
    for k in range(1, ny):
        w_one_part = w_one_part + jnp.dot(
            sens_y[k], pre_y[k], preferred_element_type=jnp.float32
        )
    w_one_part = w_one_part.reshape(nz, nc, rows_own, hidden_count)
    got = other_core(lax.dynamic_index_in_dim(w_one_part, 1 - ic, 1, False))
    sent = z_messages(ic, w_one_part, got, w_two_part, b_one_row)
    got = exchanged(sent, "z")
    grad_w_one, grad_w_two, grad_b_one = z_finished(got.astype(jnp.float32), rows_own)
    return (
        loss[0, 0] / count_all,
        grad_w_one,
        grad_b_one[0],
        grad_w_two.T,
        g_b_two[0],
        g_v_one,
        g_c_one[0],
        g_v_two,
        g_c_two[0],
        g_v_three,
        g_c_three[0],
    )


def solution(mesh):
    torus = Mesh(mesh.devices.reshape(8, 4, 2, mesh.shape["query"]), ALL)
    return jax.shard_map(
        local,
        mesh=torus,
        in_specs=(
            P(DP, None),
            P(None, "query"),
            P(DP, "query"),
            P(None, "query"),
            P("query"),
            P("query", None),
            P(),
            P(),
            P(),
            P(),
            P(),
            P(),
            P(),
        ),
        out_specs=(
            P(),
            P(DP, "query"),
            P("query"),
            P("query", DP),
            P(),
            P(),
            P(),
            P(),
            P(),
            P(),
            P(),
        ),
        check_vma=False,
    )
```

```python
import functools
import math

import jax
import jax.numpy as jnp
from jax import lax
from jax.experimental import pallas as pl
from jax.experimental.pallas import tpu as pltpu
from jax.sharding import Mesh
from jax.sharding import PartitionSpec as P


GRID = 128
BLOCK = 1024
CUT = 1024
DP = ("z", "y", "c")
ALL = ("z", "y", "c", "query")


def shift(x, axis, k):
    n = lax.axis_size(axis)
    return lax.ppermute(x, axis, [(i, (i + k) % n) for i in range(n)])


def part(x, i):
    return lax.dynamic_index_in_dim(x, i, 0, False)


def scattered_sum(chunks, axis):
    n, i = lax.axis_size(axis), lax.axis_index(axis)
    arrived = [shift(part(chunks, (i + k) % n), axis, k) for k in range(1, n)]
    total = part(chunks, i)
    for a in arrived:
        total = total + a
    return total


def exchanged(x, axis):
    return lax.all_to_all(x, axis, 0, 0, tiled=True)


def other_core(x):
    return lax.ppermute(x, "c", [(0, 1), (1, 0)])


def contract_rows(left, right, precision=None):
    return lax.dot_general(
        left,
        right,
        (((0,), (0,)), ((), ())),
        precision=precision,
        preferred_element_type=jnp.float32,
    )


def contract_cols(left, right, precision=None):
    return lax.dot_general(
        left,
        right,
        (((1,), (1,)), ((), ())),
        precision=precision,
        preferred_element_type=jnp.float32,
    )


def points_of(index):
    coords = index.astype(jnp.float32) / (GRID - 1)
    columns = jnp.concatenate([coords, jnp.zeros((6, coords.shape[1]), jnp.float32)]).T
    return columns[:, 0:1], columns[:, 1:2]


def whole(*shape):
    return pl.BlockSpec(shape, lambda i, *_: (0,) * len(shape))


def trunk_forward(query_index, v_one, c_one, v_two, c_two, v_three, c_three):
    queries = query_index.shape[1]
    trunk, basis = v_three.shape
    block = BLOCK

    def body(index, v_one, c_one, v_two, c_two, v_three, c_three, out, first_out, second_out):
        x, y = points_of(index[...])
        cuts = [slice(at, at + CUT) for at in range(0, block, CUT)]
        firsts = [
            jnp.tanh(x[c] * v_one[0:1, :] + y[c] * v_one[1:2, :] + c_one[...]) for c in cuts
        ]
        seconds = [
            jnp.dot(first.astype(jnp.bfloat16), v_two[...], preferred_element_type=jnp.float32)
            for first in firsts
        ]
        seconds = [jnp.tanh(second + c_two[...]) for second in seconds]
        for c, first, second in zip(cuts, firsts, seconds):
            first_out[c, :] = first
            second_out[c, :] = second
            full = jnp.dot(
                second.astype(jnp.bfloat16), v_three[...], preferred_element_type=jnp.float32
            )
            out[c, :] = (full + c_three[...]).astype(jnp.bfloat16)

    return pl.pallas_call(
        body,
        grid=(queries // block,),
        in_specs=[
            pl.BlockSpec((2, block), lambda i: (0, i)),
            whole(2, trunk),
            whole(1, trunk),
            whole(trunk, trunk),
            whole(1, trunk),
            whole(trunk, basis),
            whole(1, basis),
        ],
        out_specs=[
            pl.BlockSpec((block, basis), lambda i: (i, 0)),
            pl.BlockSpec((block, trunk), lambda i: (i, 0)),
            pl.BlockSpec((block, trunk), lambda i: (i, 0)),
        ],
        out_shape=[
            jax.ShapeDtypeStruct((queries, basis), jnp.bfloat16),
            jax.ShapeDtypeStruct((queries, trunk), jnp.float32),
            jax.ShapeDtypeStruct((queries, trunk), jnp.float32),
        ],
        cost_estimate=pl.CostEstimate(flops=4 * queries * trunk * basis, bytes_accessed=4_000_000, transcendentals=2 * queries * trunk),
        compiler_params=pltpu.CompilerParams(vmem_limit_bytes=60 * 2**20),
        name="trunk_forward",
    )(query_index, v_one, c_one[None], v_two, c_two[None], v_three, c_three[None])


def misfit_of(hidden_all, w_two_all, b_two, basis, targets, inv_scale, grad_scale):
    n = len(hidden_all)
    funcs, queries = targets.shape
    width = basis.shape[1]
    block = BLOCK

    def body(*refs):
        hidden, w_two = refs[:n], refs[n : 2 * n]
        b_two, basis, targets, coeffs, misfit_b, squares, grad = refs[2 * n :]

        @pl.when(pl.program_id(0) == 0)
        def _():
            total = b_two[...]
            for h, w in zip(hidden, w_two):
                total = total + jnp.dot(h[...], w[...], preferred_element_type=jnp.float32)
            coeffs[...] = total.astype(jnp.bfloat16)
            squares[...] = jnp.zeros_like(squares)
            grad[...] = jnp.zeros_like(grad)

        misfit = contract_cols(coeffs[...], basis[...]) * inv_scale - targets[...].astype(jnp.float32)
        total = jnp.sum(misfit * misfit, axis=0, keepdims=True)
        for at in range(0, block, width):
            squares[...] += total[:, at : at + width]
        scaled_b = (misfit * grad_scale).astype(jnp.bfloat16)
        misfit_b[...] = scaled_b
        grad[...] += jnp.dot(scaled_b, basis[...], preferred_element_type=jnp.float32) * inv_scale

    return pl.pallas_call(
        body,
        grid=(queries // block,),
        in_specs=[whole(*h.shape) for h in hidden_all]
        + [whole(*w.shape) for w in w_two_all]
        + [
            whole(1, width),
            pl.BlockSpec((block, width), lambda i: (i, 0)),
            pl.BlockSpec((funcs, block), lambda i: (0, i)),
        ],
        out_specs=[
            whole(funcs, width),
            pl.BlockSpec((funcs, block), lambda i: (0, i)),
            whole(1, width),
            whole(funcs, width),
        ],
        out_shape=[
            jax.ShapeDtypeStruct((funcs, width), jnp.bfloat16),
            jax.ShapeDtypeStruct((funcs, queries), jnp.bfloat16),
            jax.ShapeDtypeStruct((1, width), jnp.float32),
            jax.ShapeDtypeStruct((funcs, width), jnp.float32),
        ],
        cost_estimate=pl.CostEstimate(flops=5 * funcs * queries * width, bytes_accessed=8_000_000, transcendentals=0),
        compiler_params=pltpu.CompilerParams(vmem_limit_bytes=60 * 2**20),
        name="misfit_of",
    )(*hidden_all, *w_two_all, b_two[None], basis, targets)


def pre_of(ix, pieces, hidden, w_two):
    n = len(pieces)
    rows, basis = pieces[0].shape
    funcs, width = hidden.shape

    def body(ix, *refs):
        hidden, w_two, pre_b, bias, product, grad = refs[n:]
        for k in range(n):
            at = lax.rem(ix[0] + n - k, n) * rows
            grad[pl.ds(pl.multiple_of(at, rows), rows), :] = refs[k][...]
        act = hidden[...]
        pre = contract_cols(grad[...], w_two[...]) * (1.0 - act * act)
        pre_b[...] = pre.astype(jnp.bfloat16)
        bias[...] = jnp.sum(pre, axis=0, keepdims=True)
        product[...] = contract_rows(grad[...], act.astype(jnp.bfloat16))

    return pl.pallas_call(
        body,
        grid_spec=pltpu.PrefetchScalarGridSpec(
            num_scalar_prefetch=1,
            grid=(1,),
            in_specs=[whole(rows, basis)] * n + [whole(funcs, width), whole(width, basis)],
            out_specs=[whole(funcs, width), whole(1, width), whole(basis, width)],
            scratch_shapes=[pltpu.VMEM((funcs, basis), jnp.bfloat16)],
        ),
        out_shape=[
            jax.ShapeDtypeStruct((funcs, width), jnp.bfloat16),
            jax.ShapeDtypeStruct((1, width), jnp.float32),
            jax.ShapeDtypeStruct((basis, width), jnp.float32),
        ],
        cost_estimate=pl.CostEstimate(flops=4 * funcs * basis * width, bytes_accessed=2_000_000, transcendentals=0),
        compiler_params=pltpu.CompilerParams(vmem_limit_bytes=12 * 2**20),
        name="pre_of",
    )(ix.reshape(1), *pieces, hidden, w_two)


def columns_by_y(sensors, iy, nz, ny, width):
    funcs = sensors.shape[0]

    def body(y, src, *out):
        for k, dst in enumerate(out):
            at = lax.rem(y[0] + k, ny) * width
            dst[...] = src[:, pl.ds(pl.multiple_of(at, width), width)].T

    return pl.pallas_call(
        body,
        grid_spec=pltpu.PrefetchScalarGridSpec(
            num_scalar_prefetch=1,
            grid=(nz,),
            in_specs=[pl.BlockSpec((funcs, ny * width), lambda z, y: (0, z))],
            out_specs=[pl.BlockSpec((width, funcs), lambda z, y: (z, 0))] * ny,
        ),
        out_shape=[jax.ShapeDtypeStruct((nz * width, funcs), sensors.dtype)] * ny,
        cost_estimate=pl.CostEstimate(flops=8_000_000, bytes_accessed=4 * sensors.size, transcendentals=0),
        compiler_params=pltpu.CompilerParams(vmem_limit_bytes=60 * 2**20),
        name="columns_by_y",
    )(iy.reshape(1), sensors)


def back_kernel(core, index, misfit, coeffs, first_act, second_act, v_two, v_three, mine, give, acc3, acc2, accs, *, inv_scale):
    step = pl.program_id(0)

    @pl.when(step == 0)
    def _():
        acc3[...] = jnp.zeros_like(acc3)
        acc2[...] = jnp.zeros_like(acc2)
        accs[...] = jnp.zeros_like(accs)

    x, y = points_of(index[...])
    first, second = first_act[...], second_act[...]
    first_b, second_b = first.astype(jnp.bfloat16), second.astype(jnp.bfloat16)
    grad = contract_rows(misfit[...], coeffs[...]) * inv_scale
    grad_b = grad.astype(jnp.bfloat16)
    acc3[...] += contract_rows(second_b, grad_b)
    accs[4:5, :] += jnp.sum(grad, axis=0, keepdims=True)
    grad = contract_cols(grad_b, v_three[...]) * (1.0 - second * second)
    grad_b = grad.astype(jnp.bfloat16)
    acc2[...] += contract_rows(first_b, grad_b)
    accs[3:4, :] += jnp.sum(grad, axis=0, keepdims=True)
    grad = contract_cols(grad_b, v_two[...]) * (1.0 - first * first)
    accs[2:3, :] += jnp.sum(grad, axis=0, keepdims=True)
    accs[0:1, :] += jnp.sum(x * grad, axis=0, keepdims=True)
    accs[1:2, :] += jnp.sum(y * grad, axis=0, keepdims=True)

    rows = acc3.shape[0]

    @pl.when(step == pl.num_programs(0) - 1)
    def _():
        mine[rows:, :] = accs[...]
        give[rows:, :] = accs[...]

        @pl.when(core[0] == 0)
        def _():
            mine[:rows, :] = acc3[...]
            give[:rows, :] = acc2[...]

        @pl.when(core[0] != 0)
        def _():
            mine[:rows, :] = acc2[...]
            give[:rows, :] = acc3[...]


def trunk_backward(core, query_index, misfit_b, coeffs_b, first_act, second_act, v_two, v_three, inv_scale):
    queries = misfit_b.shape[1]
    funcs, basis = coeffs_b.shape
    trunk = v_two.shape[0]
    block = BLOCK

    out = jax.ShapeDtypeStruct((trunk + 8, basis), jnp.float32)
    return pl.pallas_call(
        functools.partial(back_kernel, inv_scale=inv_scale),
        grid_spec=pltpu.PrefetchScalarGridSpec(
            num_scalar_prefetch=1,
            grid=(queries // block,),
            in_specs=[
                pl.BlockSpec((2, block), lambda i, core: (0, i)),
                pl.BlockSpec((funcs, block), lambda i, core: (0, i)),
                whole(funcs, basis),
                pl.BlockSpec((block, trunk), lambda i, core: (i, 0)),
                pl.BlockSpec((block, trunk), lambda i, core: (i, 0)),
                whole(trunk, trunk),
                whole(trunk, basis),
            ],
            out_specs=[whole(trunk + 8, basis), whole(trunk + 8, basis)],
            scratch_shapes=[
                pltpu.VMEM((trunk, basis), jnp.float32),
                pltpu.VMEM((trunk, trunk), jnp.float32),
                pltpu.VMEM((8, basis), jnp.float32),
            ],
        ),
        out_shape=[out, out],
        cost_estimate=pl.CostEstimate(flops=12 * queries * trunk * basis, bytes_accessed=8_000_000, transcendentals=2 * queries * trunk),
        compiler_params=pltpu.CompilerParams(vmem_limit_bytes=60 * 2**20),
        name="trunk_backward",
    )(core.reshape(1), query_index, misfit_b, coeffs_b, first_act, second_act, v_two, v_three)


def scaled(x, axes=None):
    top = jnp.max(jnp.abs(x), axis=axes, keepdims=True)
    e = jnp.clip(jnp.floor(jnp.log2(jnp.maximum(top, 1e-30))), -100.0, 127.0) - 14.0
    return x * jnp.exp2(-e), e


def summed_in_pairs(x, axis):
    n, k = lax.axis_size(axis), 1
    while k < n:
        pair = k | k >> 1 if 2 * k == n else k
        x = x + lax.ppermute(x, axis, [(i, i ^ pair) for i in range(n)])
        k *= 2
    return x


def with_tail(out, j, big_e, piece, piece_e):
    rows, w = out.shape[1] - 8, out.shape[2]
    out[j, rows:, :] = jnp.zeros((8, w), jnp.float32)
    out[j, rows : rows + 1, : piece.shape[1]] = piece
    out[j, rows + 1 : rows + 2, :] = jnp.broadcast_to(big_e, (1, w))
    out[j, rows + 2 : rows + 3, :] = jnp.broadcast_to(piece_e, (1, w))


def plane_messages(mine, got, late, n):
    w = mine.shape[1]
    rows = mine.shape[0] - 8
    per = n // 8
    k = w // per

    def body(mine, got, late, out):
        big, big_e = scaled(mine[:rows, :] + got[:rows, :])
        row = lax.broadcasted_iota(jnp.int32, (8, w), 0)
        small = mine[rows:, :] + got[rows:, :]
        small = jnp.where(row == 5, late[0:1, :], jnp.where(row == 6, late[1:2, :], small))
        small, small_e = scaled(small, 1)
        out[:, : rows // n, :] = big.reshape(n, rows // n, w)
        for j in range(n):
            i, at = j // per, j % per * k
            with_tail(out, j, big_e, small[i : i + 1, at : at + k], small_e[i : i + 1])

    out = pl.pallas_call(
        body,
        out_shape=jax.ShapeDtypeStruct((n, rows // n + 8, w), jnp.float32),
        compiler_params=pltpu.CompilerParams(vmem_limit_bytes=12 * 2**20),
        name="plane_messages",
    )(mine, got, late)
    return out.astype(jnp.float16)


def plane_total(got):
    n, rows, w = got.shape[0], got.shape[1] - 8, got.shape[2]

    def body(got, out):
        def total(lo, hi, e):
            x = got[0, lo:hi, :] * jnp.exp2(got[0, e : e + 1, :])
            for j in range(1, n):
                x = x + got[j, lo:hi, :] * jnp.exp2(got[j, e : e + 1, :])
            return x

        out[:rows, :] = total(0, rows, rows + 1)
        out[rows:, :] = jnp.zeros((8, w), jnp.float32)
        out[rows : rows + 1, :] = total(rows, rows + 1, rows + 2)

    return pl.pallas_call(
        body,
        out_shape=jax.ShapeDtypeStruct((rows + 8, w), jnp.float32),
        compiler_params=pltpu.CompilerParams(vmem_limit_bytes=12 * 2**20),
        name="plane_total",
    )(got)


def total_message(both, side):
    rows, w = both.shape[0] - 8, both.shape[1]

    def body(both, out):
        big, big_e = scaled(both[:rows, :])
        small, small_e = scaled(both[rows : rows + 1, :side])
        out[0, :rows, :] = big
        with_tail(out, 0, big_e, small, small_e)

    out = pl.pallas_call(
        body,
        out_shape=jax.ShapeDtypeStruct((1, rows + 8, w), jnp.float32),
        compiler_params=pltpu.CompilerParams(vmem_limit_bytes=12 * 2**20),
        name="total_message",
    )(both)
    return out[0].astype(jnp.float16)


def z_messages(core, w_one_part, got, w_two_part, b_one_row):
    nz, _, rows, w = w_one_part.shape
    m = w_two_part.shape[1]

    def body(core, part, got, two, bias, out):
        one, one_e = scaled(part[:, 0] + got[...])
        two, two_e = scaled(two[...])
        bias, bias_e = scaled(bias[...])
        out[:, :rows, :] = one
        out[:, rows : rows + m, :] = two
        for j in range(nz):
            out[j, rows + m :, :] = jnp.zeros((8, w), jnp.float32)
            for i, row in enumerate((bias, bias_e, two_e, one_e)):
                out[j, rows + m + i : rows + m + i + 1, :] = jnp.broadcast_to(row.reshape(1, -1), (1, w))

    out = pl.pallas_call(
        body,
        grid_spec=pltpu.PrefetchScalarGridSpec(
            num_scalar_prefetch=1,
            grid=(1,),
            in_specs=[
                pl.BlockSpec((nz, 1, rows, w), lambda i, core: (0, core[0], 0, 0)),
                pl.BlockSpec((nz, rows, w), lambda i, core: (0, 0, 0)),
                pl.BlockSpec((nz, m, w), lambda i, core: (0, 0, 0)),
                pl.BlockSpec((1, w), lambda i, core: (0, 0)),
            ],
            out_specs=pl.BlockSpec((nz, rows + m + 8, w), lambda i, core: (0, 0, 0)),
        ),
        out_shape=jax.ShapeDtypeStruct((nz, rows + m + 8, w), jnp.float32),
        compiler_params=pltpu.CompilerParams(vmem_limit_bytes=12 * 2**20),
        name="z_messages",
    )(core.reshape(1), w_one_part, got, w_two_part, b_one_row)
    return out.astype(jnp.float16)


def finished(place, got, other, side):
    ny = len(got)
    nx, rows, w = got[0].shape[0], got[0].shape[1] - 8, got[0].shape[2]
    n = ny * nx
    per = n // 8

    def body(place, *refs):
        got, other = refs[:ny], refs[ny : 2 * ny]
        one, two, v_one, c_one, c_two, c_three, b_two, loss, small, more = refs[2 * ny :]

        def put(zero, last):
            for q in range(n):
                at = lax.rem(place[1] + ny - q // nx, ny) * nx + lax.rem(place[2] + nx - q % nx, nx)
                into = pl.ds(pl.multiple_of(at * rows, rows), rows)
                for refs, out, part in ((zero, one, small), (last, two, more)):
                    x, i = refs[q // nx], q % nx
                    out[into, :] = x[i, :rows, :] * jnp.exp2(x[i, rows + 1 : rows + 2, :])
                    part[pl.ds(at, 1), :] = x[i, rows : rows + 1, :side] * jnp.exp2(
                        x[i, rows + 2 : rows + 3, :side]
                    )

        @pl.when(place[0] == 0)
        def _():
            put(got, other)

        @pl.when(place[0] != 0)
        def _():
            put(other, got)

        total = jnp.zeros((1, 1), jnp.float32)
        for p in range(per):
            at = slice(p * side, (p + 1) * side)
            for i, (out, j) in enumerate(((v_one, 0), (v_one, 1), (c_one, 0), (c_two, 0), (c_three, 0))):
                out[j : j + 1, at] = small[i * per + p : i * per + p + 1, :]
            k = 5 * per + p
            b_two[:, at] = small[k : k + 1, :] + more[k : k + 1, :]
            k = 6 * per + p
            total = total + jnp.sum(small[k : k + 1, :] + more[k : k + 1, :], axis=1, keepdims=True)
        loss[...] = total

    shapes = [(n * rows, w), (n * rows, w), (2, w)] + [(1, w)] * 4 + [(1, 1)]
    return pl.pallas_call(
        body,
        grid_spec=pltpu.PrefetchScalarGridSpec(
            num_scalar_prefetch=1,
            grid=(1,),
            in_specs=[whole(*x.shape) for x in (*got, *other)],
            out_specs=[whole(*shape) for shape in shapes],
            scratch_shapes=[pltpu.VMEM((n, side), jnp.float32)] * 2,
        ),
        out_shape=[jax.ShapeDtypeStruct(shape, jnp.float32) for shape in shapes],
        compiler_params=pltpu.CompilerParams(vmem_limit_bytes=24 * 2**20),
        name="finished",
    )(place, *got, *other)


def z_finished(got, rows):
    nz, all_rows, w = got.shape
    m = all_rows - rows - 8

    def body(got, one, two, bias):
        def part(lo, hi, e):
            total = got[0, lo:hi, :] * jnp.exp2(got[0, e : e + 1, :])
            for j in range(1, nz):
                total = total + got[j, lo:hi, :] * jnp.exp2(got[j, e : e + 1, :])
            return total

        k = rows + m
        one[...] = part(0, rows, k + 3)
        two[...] = part(rows, k, k + 2)
        bias[...] = part(k, k + 1, k + 1)

    return pl.pallas_call(
        body,
        out_shape=[jax.ShapeDtypeStruct(shape, jnp.float32) for shape in ((rows, w), (m, w), (1, w))],
        compiler_params=pltpu.CompilerParams(vmem_limit_bytes=12 * 2**20),
        name="z_finished",
    )(got)


def sum_of_all(mine, give, b_two, squares):
    w = mine.shape[1]
    ny, nx = lax.axis_size("y"), lax.axis_size("query")
    n = ny * nx
    side = 8 * w // n
    got = other_core(give)

    got = exchanged(plane_messages(mine, got, jnp.concatenate([b_two, squares]), n), ("y", "query"))
    both = plane_total(got.astype(jnp.float32))
    both = summed_in_pairs(both, "z")
    got = total_message(both, side)
    got = jnp.stack([got] + [shift(got, "query", k) for k in range(1, nx)])
    pieces = [got] + [shift(got, "y", k) for k in range(1, ny)]
    others = [other_core(p) for p in pieces]
    place = jnp.stack([lax.axis_index(a) for a in ("c", "y", "query")])
    return finished(
        place,
        [p.astype(jnp.float32) for p in pieces],
        [p.astype(jnp.float32) for p in others],
        side,
    )


def local(
    sensors,
    query_index,
    targets,
    w_one,
    b_one,
    w_two,
    b_two,
    v_one,
    c_one,
    v_two,
    c_two,
    v_three,
    c_three,
):
    funcs, sensor_count = sensors.shape
    hidden_count, basis_count = w_two.shape
    query_rows = query_index.shape[1]
    nz, ny, nc, nx = (lax.axis_size(a) for a in ALL)
    count_all = funcs * nz * ny * nc * query_rows * nx
    grad_scale = 64.0 / math.sqrt(count_all)
    inv_scale = 1.0 / math.sqrt(basis_count)

    w_two_all = [w_two] + [shift(w_two, "query", k) for k in range(1, nx)]
    hidden = jnp.tanh(jnp.dot(sensors, w_one, preferred_element_type=jnp.float32) + b_one)
    hidden_b = hidden.astype(jnp.bfloat16)
    hidden_all = [hidden_b] + [shift(hidden_b, "query", k) for k in range(1, nx)]
    basis, first_act, second_act = trunk_forward(
        query_index, v_one, c_one, v_two, c_two, v_three, c_three
    )

    rows_own = sensor_count // (nz * ny * nc)
    iy, ic = lax.axis_index("y"), lax.axis_index("c")
    sensors_late, _ = lax.optimization_barrier((sensors, hidden_b))
    sens_y = columns_by_y(sensors_late, iy, nz, ny, nc * rows_own)
    sens_y = [sens_y[0]] + [shift(sens_y[k], "y", k) for k in range(1, ny)]

    coeffs_b, misfit_b, squares, grad_part = misfit_of(
        hidden_all, w_two_all, b_two, basis, targets, inv_scale, grad_scale
    )
    grad_own = exchanged(grad_part.reshape(nx, -1, basis_count), "query")
    grad_own = jnp.sum(grad_own, axis=0)
    b_two_part = jnp.sum(grad_own, axis=0, keepdims=True)
    grad_own_b = grad_own.astype(jnp.bfloat16)
    grad_pieces = [grad_own_b] + [shift(grad_own_b, "query", k) for k in range(1, nx)]

    mine, give = trunk_backward(ic, query_index, misfit_b, coeffs_b, first_act, second_act, v_two, v_three, inv_scale)
    totals = sum_of_all(mine, give, b_two_part, squares)
    g_v_three, g_v_two, g_v_one, g_c_one, g_c_two, g_c_three, g_b_two, loss = totals

    grad_pre_b, b_one_part, w_two_part = pre_of(
        lax.axis_index("query"), grad_pieces, hidden, w_two
    )

    pre_y = [grad_pre_b] + [shift(grad_pre_b, "y", k) for k in range(1, ny)]

    w_two_part = w_two_part.reshape(nz, ny, nc, -1, hidden_count)
    b_one_rows = jnp.pad(b_one_part, ((0, 7), (0, 0)))

    def with_bias(rows, n):
        rows = rows.reshape(n, -1, hidden_count)
        bias = jnp.broadcast_to(b_one_rows, (n, 8, hidden_count))
        return jnp.concatenate([rows, bias], axis=1)

    both = scattered_sum(with_bias(w_two_part.transpose(2, 0, 1, 3, 4), nc), "c")
    w_two_part, b_one_rows = both[:-8].reshape(nz, ny, -1, hidden_count), both[-8:]
    both = scattered_sum(with_bias(w_two_part.transpose(1, 0, 2, 3), ny), "y")
    w_two_part, b_one_row = both[:-8].reshape(nz, -1, hidden_count), both[-8:-7]

    w_one_part = jnp.dot(sens_y[0], pre_y[0], preferred_element_type=jnp.float32)
    for k in range(1, ny):
        w_one_part = w_one_part + jnp.dot(
            sens_y[k], pre_y[k], preferred_element_type=jnp.float32
        )
    w_one_part = w_one_part.reshape(nz, nc, rows_own, hidden_count)
    got = other_core(lax.dynamic_index_in_dim(w_one_part, 1 - ic, 1, False))
    sent = z_messages(ic, w_one_part, got, w_two_part, b_one_row)
    got = exchanged(sent, "z")
    grad_w_one, grad_w_two, grad_b_one = z_finished(got.astype(jnp.float32), rows_own)
    return (
        loss[0, 0] / count_all,
        grad_w_one,
        grad_b_one[0],
        grad_w_two.T,
        g_b_two[0],
        g_v_one,
        g_c_one[0],
        g_v_two,
        g_c_two[0],
        g_v_three,
        g_c_three[0],
    )


def solution(mesh):
    torus = Mesh(mesh.devices.reshape(8, 4, 2, mesh.shape["query"]), ALL)
    return jax.shard_map(
        local,
        mesh=torus,
        in_specs=(
            P(DP, None),
            P(None, "query"),
            P(DP, "query"),
            P(None, "query"),
            P("query"),
            P("query", None),
            P(),
            P(),
            P(),
            P(),
            P(),
            P(),
            P(),
        ),
        out_specs=(
            P(),
            P(DP, "query"),
            P("query"),
            P("query", DP),
            P(),
            P(),
            P(),
            P(),
            P(),
            P(),
            P(),
        ),
        check_vma=False,
    )
```
